512 devices in a mesh: row: 32 (over x, z_lo, core), col: 16 (over y, z_hi).
Axes of the slice: x: 4, y: 8, z: 8 (z_hi: 2, z_lo: 4; z = z_hi * 4 + z_lo), core: 2. Of those that a mesh axis runs over, the one named last changes fastest.
Arguments:
- tokens: bfloat16 [192, 8192], P('row', 'col'), may hold values from -6 to 6
- gate_weight: bfloat16 [8192, 20480], P('col', 'row'), may hold values from -0.0625 to 0.0625
- up_weight: bfloat16 [8192, 20480], P('col', 'row'), may hold values from -0.0625 to 0.0625
- down_weight: bfloat16 [20480, 8192], P('row', 'col'), may hold values from -0.0390625 to 0.0390625
- keep_mask: int32 [192, 20480], P('col', 'row'), may hold values 0 or 1
- cotangent: bfloat16 [192, 8192], P('row', 'col'), may hold values from -6 to 6
Outputs:
- mixed_out: bfloat16 [192, 8192], P('row', 'col')
- input_grad: bfloat16 [192, 8192], P('row', 'col')
- gate_grad: bfloat16 [8192, 20480], P('col', 'row')
- up_grad: bfloat16 [8192, 20480], P('col', 'row')
- down_grad: bfloat16 [20480, 8192], P('row', 'col')
The draws below stay inside these ranges and needn't reach their ends.
All inputs are finite; a program needn't handle non-finite values. No bound on the sum of `keep_mask` on one device may be relied on, other than what follows from the above.
Results may differ from the reference program's by a relative error of at most 0.0049.
Values may be sent and summed in bfloat16 or wider, within the bound.
No kernel may reach another device: no remote copies, remote signals or barrier semaphores. Data moves between devices by JAX's collectives and lax.ppermute only.
A program may use at most 64 MiB of HBM per device.

```python
import jax
import jax.numpy as jnp

D = 8192
FF = 20480
TOKENS = 192


def with_ends(result, key, smallest, largest):
    shape = result.shape
    spot = [jax.random.randint(jax.random.fold_in(key, axis), (), 0, shape[axis]) for axis in range(len(shape))]
    result = result.at[tuple(spot)].set(smallest)
    longest = shape.index(max(shape))
    spot[longest] = (spot[longest] + 1) % shape[longest]
    return result.at[tuple(spot)].set(largest)


def block_scale(rng, extent, pieces, low, largest):
    gain = 1.0
    for axis_at, parts in pieces:
        draws = jax.random.uniform(jax.random.fold_in(jax.random.fold_in(rng, 6), axis_at), (parts,), jnp.float32, low / len(pieces), largest / len(pieces))
        gain = gain * jnp.repeat(jnp.exp(draws), extent[axis_at] // parts).reshape((-1,) + (1,) * (len(extent) - 1 - axis_at))
    return gain


def normal_values(stream_key, shape, deviation, most, cuts=(), kind=jnp.bfloat16):
    entries = deviation * jax.random.normal(stream_key, shape, jnp.float32)
    if cuts:
        entries = entries * block_scale(stream_key, shape, cuts, -0.22, 0.18)
    return jnp.clip(entries, -most, most).astype(kind)


def setup_inputs(seed: int = 0) -> dict:
    streams_of = jax.random.split(jax.random.key(seed), 7)
    return {
        "tokens": normal_values(streams_of[0], (TOKENS, D), 1.0, 6.0, ((0, 32), (1, 16))),
        "gate_weight": normal_values(streams_of[1], (D, FF), D ** -0.5, 0.0625, ((0, 16), (1, 32))),
        "up_weight": normal_values(streams_of[2], (D, FF), D ** -0.5, 0.0625, ((0, 16), (1, 32))),
        "down_weight": normal_values(streams_of[3], (FF, D), FF ** -0.5, 0.0390625, ((0, 32), (1, 16))),
        "keep_mask": with_ends((jax.random.randint(streams_of[4], (TOKENS, FF), 0, 10) < 9).astype(jnp.int32), jax.random.fold_in(streams_of[4], 1), 0, 1),
        "cotangent": normal_values(streams_of[5], (TOKENS, D), 1.0, 6.0, ((0, 32), (1, 16))),
    }


keep_scale = 1.0 / 0.9


def reference(tokens, gate_weight, up_weight, down_weight, keep_mask, cotangent):
    gate_value = jnp.dot(tokens, gate_weight, preferred_element_type=jnp.float32)
    up_value = jnp.dot(tokens, up_weight, preferred_element_type=jnp.float32)
    keep_factor = keep_mask.astype(jnp.float32) * keep_scale
    sigmoid_gate = jax.nn.sigmoid(gate_value)
    silu_gate = gate_value * sigmoid_gate
    hidden = (silu_gate * up_value * keep_factor).astype(jnp.bfloat16)
    mixed_out = jnp.dot(hidden, down_weight, preferred_element_type=jnp.float32).astype(jnp.bfloat16)
    grad_hidden = jnp.dot(cotangent, down_weight.T, preferred_element_type=jnp.float32)
    down_grad = jnp.dot(hidden.T, cotangent, preferred_element_type=jnp.float32).astype(jnp.bfloat16)
    grad_pre = grad_hidden * keep_factor
    grad_gate = (grad_pre * up_value * sigmoid_gate * (1.0 + gate_value * (1.0 - sigmoid_gate))).astype(jnp.bfloat16)
    grad_up = (grad_pre * silu_gate).astype(jnp.bfloat16)
    gate_grad = jnp.dot(tokens.T, grad_gate, preferred_element_type=jnp.float32).astype(jnp.bfloat16)
    up_grad = jnp.dot(tokens.T, grad_up, preferred_element_type=jnp.float32).astype(jnp.bfloat16)
    input_sum = jnp.dot(grad_gate, gate_weight.T, preferred_element_type=jnp.float32)
    input_sum = input_sum + jnp.dot(grad_up, up_weight.T, preferred_element_type=jnp.float32)
    input_grad = input_sum.astype(jnp.bfloat16)
    return mixed_out, input_grad, gate_grad, up_grad, down_grad
```

```python
import jax
import jax.numpy as jnp
from jax import lax
from jax.sharding import PartitionSpec as P

keep_scale = 1.0 / 0.9
contract_last = (((1,), (1,)), ((), ()))
contract_first = (((0,), (0,)), ((), ()))
lanes = 128


def exchange(blocks, axis):
    return lax.all_to_all(blocks, axis, split_axis=0, concat_axis=0, tiled=True)


def sent_to_all(block, axis):
    copies = jnp.broadcast_to(block, (lax.axis_size(axis), *block.shape))
    return exchange(copies, axis)


def dot(a, b, dims=(((1,), (0,)), ((), ()))):
    return lax.dot_general(a, b, dims, preferred_element_type=jnp.float32)


def body(tokens, gate_weight, up_weight, down_weight, keep_mask, cotangent):
    bf16 = jnp.bfloat16
    rows, cols = lax.axis_size("row"), lax.axis_size("col")
    own, width = tokens.shape
    total = own * rows
    share, units = keep_mask.shape

    packed = jnp.concatenate([tokens.reshape(-1, lanes), cotangent.reshape(-1, lanes)], axis=0)
    arrived = sent_to_all(packed, "row")
    half = packed.shape[0] // 2
    all_tokens = arrived[:, :half].reshape(total, width)
    all_cot = arrived[:, half:].reshape(total, width)

    parts = [
        dot(all_tokens, gate_weight),
        dot(all_tokens, up_weight),
        dot(all_cot, down_weight, contract_last),
    ]
    parts = jnp.concatenate([p.astype(bf16).reshape(cols, share, units) for p in parts], axis=1)
    sums = exchange(parts, "col").astype(jnp.float32).sum(axis=0)
    gate_value, up_value, grad_hidden = jnp.split(sums, 3, axis=0)

    keep_factor = keep_mask.astype(jnp.float32) * keep_scale
    sigmoid_gate = jax.nn.sigmoid(gate_value)
    silu_gate = gate_value * sigmoid_gate
    hidden = silu_gate * up_value * keep_factor
    grad_pre = grad_hidden * keep_factor
    grad_gate = grad_pre * up_value * sigmoid_gate * (1.0 + gate_value * (1.0 - sigmoid_gate))
    grad_up = grad_pre * silu_gate
    mine = jnp.concatenate([hidden, grad_gate, grad_up], axis=0).astype(bf16)
    spread = sent_to_all(mine, "col")
    hidden_all, gate_all, up_all = (a.reshape(total, units) for a in jnp.split(spread, 3, axis=1))

    out_part = dot(hidden_all, down_weight).astype(bf16)
    in_part = (
        dot(gate_all, gate_weight, contract_last) + dot(up_all, up_weight, contract_last)
    ).astype(bf16)
    parts = jnp.concatenate([p.reshape(rows, -1, lanes) for p in (out_part, in_part)], axis=1)
    sums = exchange(parts, "row").astype(jnp.float32).sum(axis=0).astype(bf16)
    mixed_out, input_grad = (a.reshape(own, width) for a in jnp.split(sums, 2, axis=0))

    down_grad = dot(hidden_all, all_cot, contract_first).astype(bf16)
    gate_grad = dot(all_tokens, gate_all, contract_first).astype(bf16)
    up_grad = dot(all_tokens, up_all, contract_first).astype(bf16)
    return (mixed_out, input_grad, gate_grad, up_grad, down_grad)


def solution(mesh):
    by_row, by_col = P("row", "col"), P("col", "row")
    return jax.shard_map(
        body,
        mesh=mesh,
        in_specs=(by_row, by_col, by_col, by_row, by_col, by_row),
        out_specs=(by_row, by_row, by_col, by_col, by_row),
        check_vma=False,
    )
```

```python
import jax
import jax.numpy as jnp
from jax import lax
from jax.sharding import Mesh
from jax.sharding import PartitionSpec as P

keep_scale = 1.0 / 0.9
contract_last = (((1,), (1,)), ((), ()))
contract_first = (((0,), (0,)), ((), ()))
lanes = 128
plane = ("x", "zl")


def exchange(blocks, axis):
    return lax.all_to_all(blocks, axis, split_axis=0, concat_axis=0, tiled=True)


def sent_to_all(block, axis):
    copies = jnp.broadcast_to(block, (lax.axis_size(axis), *block.shape))
    return exchange(copies, axis)


def swapped(value, axis):
    return lax.ppermute(value, axis, [(0, 1), (1, 0)])


def in_order(mine, other, axis, dim):
    first = lax.axis_index(axis) == 0
    a, b = jnp.where(first, mine, other), jnp.where(first, other, mine)
    return jnp.stack([a, b], axis=dim)


def dot(a, b, dims=(((1,), (0,)), ((), ()))):
    return lax.dot_general(a, b, dims, preferred_element_type=jnp.float32)


def body(tokens, gate_weight, up_weight, down_weight, keep_mask, cotangent):
    bf16, f32 = jnp.bfloat16, jnp.float32
    own, width = tokens.shape
    share, units = keep_mask.shape
    ring = lax.axis_size("y")
    total = share * 2 * ring
    chips = total // own // 2

    packed = jnp.concatenate([tokens.reshape(-1, lanes), cotangent.reshape(-1, lanes)], axis=0)
    half = packed.shape[0] // 2
    near = sent_to_all(packed, plane)
    both = in_order(near, swapped(near, "core"), "core", 1)
    all_tokens = both[:, :, :half].reshape(total, width)
    all_cot = both[:, :, half:].reshape(total, width)

    parts = [
        dot(all_tokens, gate_weight),
        dot(all_tokens, up_weight),
        dot(all_cot, down_weight, contract_last),
    ]
    parts = jnp.concatenate([p.astype(bf16).reshape(ring, 2 * share, units) for p in parts], axis=1)
    sums = exchange(parts, "y").astype(f32).sum(axis=0)
    sums = sums + swapped(sums, "zh")
    gate_value, up_value, grad_hidden = jnp.split(sums, 3, axis=0)

    keep = keep_mask.astype(bf16)
    keep = in_order(keep, swapped(keep, "zh"), "zh", 0).reshape(2 * share, units)
    keep_factor = keep.astype(f32) * keep_scale
    sigmoid_gate = jax.nn.sigmoid(gate_value)
    silu_gate = gate_value * sigmoid_gate
    hidden = silu_gate * up_value * keep_factor
    grad_pre = grad_hidden * keep_factor
    grad_gate = grad_pre * up_value * sigmoid_gate * (1.0 + gate_value * (1.0 - sigmoid_gate))
    grad_up = grad_pre * silu_gate
    mine = jnp.concatenate([hidden, grad_gate, grad_up], axis=0).astype(bf16)
    spread = sent_to_all(mine, "y")
    hidden_all, gate_all, up_all = (a.reshape(total, units) for a in jnp.split(spread, 3, axis=1))

    out_part = dot(hidden_all, down_weight)
    in_part = dot(gate_all, gate_weight, contract_last) + dot(up_all, up_weight, contract_last)
    parts = jnp.stack([p.reshape(chips, 2, -1, lanes) for p in (out_part, in_part)], axis=2)
    core = lax.axis_index("core")
    kept = jnp.where(core == 0, parts[:, 0], parts[:, 1])
    given = jnp.where(core == 0, parts[:, 1], parts[:, 0])
    parts = (kept + swapped(given, "core")).astype(bf16).reshape(chips, -1, lanes)
    sums = exchange(parts, plane).astype(f32).sum(axis=0).astype(bf16)
    mixed_out, input_grad = (a.reshape(own, width) for a in jnp.split(sums, 2, axis=0))

    down_grad = dot(hidden_all, all_cot, contract_first).astype(bf16)
    gate_grad = dot(all_tokens, gate_all, contract_first).astype(bf16)
    up_grad = dot(all_tokens, up_all, contract_first).astype(bf16)
    return (mixed_out, input_grad, gate_grad, up_grad, down_grad)


def solution(mesh):
    fine = Mesh(mesh.devices.reshape(4, 4, 2, 8, 2), ("x", "zl", "core", "y", "zh"))
    row, col = ("x", "zl", "core"), ("y", "zh")
    by_row, by_col = P(row, col), P(col, row)
    return jax.shard_map(
        body,
        mesh=fine,
        in_specs=(by_row, by_col, by_col, by_row, by_col, by_row),
        out_specs=(by_row, by_row, by_col, by_col, by_row),
        check_vma=False,
    )
```

```python
import jax
import jax.numpy as jnp
from jax import lax
from jax.experimental import pallas as pl
from jax.experimental.pallas import tpu as pltpu
from jax.sharding import Mesh
from jax.sharding import PartitionSpec as P

keep_scale = 1.0 / 0.9
contract_last = (((1,), (1,)), ((), ()))
contract_first = (((0,), (0,)), ((), ()))
lanes = 128
plane = ("x", "zl")


def exchange(blocks, axis):
    return lax.all_to_all(blocks, axis, split_axis=0, concat_axis=0, tiled=True)


def sent_to_all(block, axis):
    copies = jnp.broadcast_to(block, (lax.axis_size(axis), *block.shape))
    return exchange(copies, axis)


def swapped(value, axis):
    return lax.ppermute(value, axis, [(0, 1), (1, 0)])


def in_order(mine, other, first, dim):
    a, b = jnp.where(first, mine, other), jnp.where(first, other, mine)
    return jnp.stack([a, b], axis=dim)


def dot(a, b, dims=(((1,), (0,)), ((), ()))):
    return lax.dot_general(a, b, dims, preferred_element_type=jnp.float32)


def products(tokens, cotangent, gate_weight, up_weight, down_weight, keep_mask, ring):
    total, units = tokens.shape[0], gate_weight.shape[1]
    rows = total // ring

    def kernel(t_ref, c_ref, g_ref, u_ref, d_ref, k_ref, out_ref, keep_ref):
        def put(at, value):
            value = value.astype(out_ref.dtype)
            for y in range(ring):
                out_ref[y, at * rows : (at + 1) * rows, :] = value[y * rows : (y + 1) * rows]

        keep_ref[...] = k_ref[...].astype(jnp.float32)
        put(0, dot(t_ref[...], g_ref[...]))
        put(1, dot(t_ref[...], u_ref[...]))
        put(2, dot(c_ref[...], d_ref[...], contract_last))

    operands = (tokens, cotangent, gate_weight, up_weight, down_weight, keep_mask)
    operands = tuple(pltpu.with_memory_space_constraint(a, pltpu.VMEM) for a in operands)
    in_vmem = pl.BlockSpec(memory_space=pltpu.VMEM)
    return pl.pallas_call(
        kernel,
        out_shape=(
            pltpu.VMEM((ring, 3 * rows, units), tokens.dtype),
            pltpu.VMEM(keep_mask.shape, jnp.float32),
        ),
        in_specs=[in_vmem] * len(operands),
        out_specs=(in_vmem, in_vmem),
        cost_estimate=pl.CostEstimate(
            flops=6 * total * tokens.shape[1] * units,
            bytes_accessed=sum(2 * a.size for a in operands),
            transcendentals=0,
        ),
        compiler_params=pltpu.CompilerParams(vmem_limit_bytes=8 << 20),
        name="products",
    )(*operands)


def body(tokens, gate_weight, up_weight, down_weight, keep_mask, cotangent):
    bf16, f32 = jnp.bfloat16, jnp.float32
    own, width = tokens.shape
    share, units = keep_mask.shape
    ring = lax.axis_size("y")
    total = share * 2 * ring
    chips = total // own // 2

    packed = jnp.concatenate([tokens, cotangent], axis=0).reshape(-1, lanes)
    half = packed.shape[0] // 2
    places = lax.axis_index("core"), lax.axis_index("zh")
    packed, core, side = lax.optimization_barrier((packed, *places))
    near = sent_to_all(packed, plane)
    both = in_order(near, swapped(near, "core"), core == 0, 1)
    all_tokens = both[:, :, :half].reshape(total, width)
    all_cot = both[:, :, half:].reshape(total, width)

    parts, keep = products(all_tokens, all_cot, gate_weight, up_weight, down_weight, keep_mask, ring)
    sums = exchange(parts, "y").astype(f32).sum(axis=0)
    other = swapped(jnp.concatenate([sums, keep], axis=0), "zh")
    sums = sums + other[: sums.shape[0]]
    keep = in_order(keep, other[sums.shape[0] :], side == 0, 0).reshape(2 * share, units)
    gate_value, up_value, grad_hidden = jnp.split(sums, 3, axis=0)

    keep_factor = keep * keep_scale
    sigmoid_gate = jax.nn.sigmoid(gate_value)
    silu_gate = gate_value * sigmoid_gate
    hidden = silu_gate * up_value * keep_factor
    grad_pre = grad_hidden * keep_factor
    grad_gate = grad_pre * up_value * sigmoid_gate * (1.0 + gate_value * (1.0 - sigmoid_gate))
    grad_up = grad_pre * silu_gate
    mine = jnp.concatenate([hidden, grad_gate, grad_up], axis=0).astype(bf16)
    spread = sent_to_all(mine, "y")
    hidden_all, gate_all, up_all = (a.reshape(total, units) for a in jnp.split(spread, 3, axis=1))

    out_part = dot(hidden_all, down_weight)
    in_part = dot(gate_all, gate_weight, contract_last) + dot(up_all, up_weight, contract_last)
    parts = jnp.stack([p.reshape(chips, 2, -1, lanes) for p in (out_part, in_part)], axis=2)
    kept = jnp.where(core == 0, parts[:, 0], parts[:, 1])
    given = jnp.where(core == 0, parts[:, 1], parts[:, 0])
    parts = (kept + swapped(given, "core")).astype(bf16).reshape(chips, -1, lanes)
    sums = exchange(parts, plane).astype(f32).sum(axis=0).astype(bf16)
    mixed_out, input_grad = jnp.split(sums.reshape(2 * own, width), 2, axis=0)

    down_grad = dot(hidden_all, all_cot, contract_first).astype(bf16)
    gate_grad = dot(all_tokens, gate_all, contract_first).astype(bf16)
    up_grad = dot(all_tokens, up_all, contract_first).astype(bf16)
    return (mixed_out, input_grad, gate_grad, up_grad, down_grad)


def solution(mesh):
    fine = Mesh(mesh.devices.reshape(4, 4, 2, 8, 2), ("x", "zl", "core", "y", "zh"))
    row, col = ("x", "zl", "core"), ("y", "zh")
    by_row, by_col = P(row, col), P(col, row)
    return jax.shard_map(
        body,
        mesh=fine,
        in_specs=(by_row, by_col, by_col, by_row, by_col, by_row),
        out_specs=(by_row, by_row, by_col, by_col, by_row),
        check_vma=False,
    )
```

```python
import jax
import jax.numpy as jnp
from jax import lax
from jax.experimental import pallas as pl
from jax.experimental.pallas import tpu as pltpu
from jax.sharding import Mesh
from jax.sharding import PartitionSpec as P

keep_scale = 1.0 / 0.9
contract_last = (((1,), (1,)), ((), ()))
contract_first = (((0,), (0,)), ((), ()))
lanes = 128
plane = ("x", "zl")


def exchange(blocks, axis):
    return lax.all_to_all(blocks, axis, split_axis=0, concat_axis=0, tiled=True)


def sent_to_all(block, axis):
    copies = jnp.broadcast_to(block, (lax.axis_size(axis), *block.shape))
    return exchange(copies, axis)


def swapped(value, axis):
    return lax.ppermute(value, axis, [(0, 1), (1, 0)])


def in_order(mine, other, first, dim):
    a, b = jnp.where(first, mine, other), jnp.where(first, other, mine)
    return jnp.stack([a, b], axis=dim)


def dot(a, b, dims=(((1,), (0,)), ((), ()))):
    return lax.dot_general(a, b, dims, preferred_element_type=jnp.float32)


def vmem_call(kernel, operands, outs, flops, scratch=(), limit=8 << 20, out_space=pltpu.VMEM):
    space, to = (pl.BlockSpec(memory_space=m) for m in (pltpu.VMEM, out_space))
    read = 4 * sum(a.size for a in operands)
    operands = [pltpu.with_memory_space_constraint(a, pltpu.VMEM) for a in operands]
    return pl.pallas_call(
        kernel,
        out_shape=tuple(out_space(*o) for o in outs),
        in_specs=[space] * len(operands),
        out_specs=(to,) * len(outs),
        scratch_shapes=scratch,
        cost_estimate=pl.CostEstimate(flops=flops, bytes_accessed=read, transcendentals=0),
        compiler_params=pltpu.CompilerParams(vmem_limit_bytes=limit),
    )(*operands)


def read_weights(near, weights, keep_mask):
    def kernel(n_ref, g_hbm, u_hbm, d_hbm, k_hbm, g_ref, u_ref, d_ref, keep_ref, mask, sems):
        pairs = ((g_hbm, g_ref), (u_hbm, u_ref), (d_hbm, d_ref), (k_hbm, mask))
        moves = [pltpu.make_async_copy(*pair, sems.at[i]) for i, pair in enumerate(pairs)]
        for move in moves:
            move.start()
        moves[3].wait()
        keep_ref[...] = mask[...].astype(jnp.float32)
        for move in moves[:3]:
            move.wait()

    space, far = (pl.BlockSpec(memory_space=m) for m in (pltpu.VMEM, pltpu.HBM))
    operands = [pltpu.with_memory_space_constraint(a, pltpu.HBM) for a in (*weights, keep_mask)]
    return pl.pallas_call(
        kernel,
        out_shape=(
            *(pltpu.VMEM(w.shape, w.dtype) for w in weights),
            pltpu.VMEM(keep_mask.shape, jnp.float32),
        ),
        in_specs=[space, far, far, far, far],
        out_specs=(space,) * 4,
        scratch_shapes=[
            pltpu.VMEM(keep_mask.shape, keep_mask.dtype),
            pltpu.SemaphoreType.DMA((4,)),
        ],
        cost_estimate=pl.CostEstimate(flops=10**9, bytes_accessed=2 << 20, transcendentals=0),
        compiler_params=pltpu.CompilerParams(vmem_limit_bytes=4 << 20),
        name="read_weights",
    )(near, *operands)


def back_products(spread, weights):
    _, _, down_weight = weights
    ring, rows, units = spread.shape
    rows = rows // 3
    total, width = ring * rows, down_weight.shape[1]

    def kernel(s_ref, g_ref, u_ref, d_ref, out_ref):
        hidden, gate, up = (
            s_ref[:, m * rows : (m + 1) * rows, :].reshape(total, units) for m in range(3)
        )
        out_ref[0] = dot(hidden, d_ref[...])
        out_ref[1] = dot(gate, g_ref[...], contract_last) + dot(up, u_ref[...], contract_last)

    outs = (((2, total, width), jnp.float32),)
    flops = 6 * total * width * units
    return vmem_call(kernel, (spread, *weights), outs, flops)[0]


def weight_gradients(spread, tokens, cotangent):
    _, rows, units = spread.shape
    rows = rows // 3
    total, width = tokens.shape

    def kernel(s_ref, t_ref, c_ref, down_hbm, gate_hbm, up_hbm, down_ref, gate_ref, up_ref, sems):
        hidden, gate, up = (
            s_ref[:, m * rows : (m + 1) * rows, :].reshape(total, units) for m in range(3)
        )
        jobs = (
            (gate_ref, gate_hbm, t_ref, gate),
            (up_ref, up_hbm, t_ref, up),
            (down_ref, down_hbm, None, None),
        )
        moves = []
        for i, (ref, hbm, x_ref, y) in enumerate(jobs):
            x, y = (hidden, c_ref[...]) if x_ref is None else (x_ref[...], y)
            ref[...] = dot(x, y, contract_first).astype(ref.dtype)
            moves.append(pltpu.make_async_copy(ref, hbm, sems.at[i]))
            moves[i].start()
        for move in moves:
            move.wait()

    kind = tokens.dtype
    outs = (((units, width), kind), ((width, units), kind), ((width, units), kind))
    scratch = [*(pltpu.VMEM(*o) for o in outs), pltpu.SemaphoreType.DMA((3,))]
    flops = 6 * total * width * units
    return vmem_call(kernel, (spread, tokens, cotangent), outs, flops, scratch, out_space=pltpu.HBM)


def own_outputs(arrived, own, width):
    def kernel(a_ref, out_ref, in_ref, flat):
        flat[...] = a_ref[...].astype(jnp.float32).sum(axis=0)
        for ref, start in ((out_ref, 0), (in_ref, flat.shape[0] // 2)):
            for c in range(width // lanes):
                piece = flat[pl.ds(start + c, own, stride=width // lanes), :]
                ref[:, c * lanes : (c + 1) * lanes] = piece.astype(ref.dtype)

    space = pl.BlockSpec(memory_space=pltpu.VMEM)
    out = jax.ShapeDtypeStruct((own, width), arrived.dtype)
    return pl.pallas_call(
        kernel,
        out_shape=(out, out),
        in_specs=[space],
        out_specs=(space, space),
        scratch_shapes=[pltpu.VMEM(arrived.shape[1:], jnp.float32)],
        compiler_params=pltpu.CompilerParams(vmem_limit_bytes=4 << 20),
        name="own_outputs",
    )(pltpu.with_memory_space_constraint(arrived, pltpu.VMEM))


def products(tokens, cotangent, weights, ring):
    total, units = tokens.shape[0], weights[0].shape[1]
    rows = total // ring

    def kernel(t_ref, c_ref, g_ref, u_ref, d_ref, out_ref):
        def put(at, value):
            value = value.astype(out_ref.dtype).reshape(ring, rows, units)
            out_ref[:, at * rows : (at + 1) * rows, :] = value

        put(0, dot(t_ref[...], g_ref[...]))
        put(1, dot(t_ref[...], u_ref[...]))
        put(2, dot(c_ref[...], d_ref[...], contract_last))

    outs = (((ring, 3 * rows, units), tokens.dtype),)
    flops = 6 * tokens.size * units
    return vmem_call(kernel, (tokens, cotangent, *weights), outs, flops)[0]


def body(tokens, gate_weight, up_weight, down_weight, keep_mask, cotangent):
    bf16, f32 = jnp.bfloat16, jnp.float32
    own, width = tokens.shape
    share, units = keep_mask.shape
    ring = lax.axis_size("y")
    total = share * 2 * ring
    chips = total // own // 2

    packed = jnp.concatenate([tokens, cotangent], axis=0).reshape(-1, lanes)
    half = packed.shape[0] // 2
    first_core, first_side = lax.axis_index("core") == 0, lax.axis_index("zh") == 0
    packed, first_core, first_side = lax.optimization_barrier((packed, first_core, first_side))
    near = sent_to_all(packed, plane)
    weights = (gate_weight, up_weight, down_weight)
    other = swapped(near, "core")
    *weights, keep = read_weights(near[0, :8], weights, keep_mask)
    both = in_order(near, other, first_core, 1)
    all_tokens = both[:, :, :half].reshape(total, width)
    all_cot = both[:, :, half:].reshape(total, width)

    parts = products(all_tokens, all_cot, weights, ring)
    sums = exchange(parts, "y").astype(f32).sum(axis=0)
    other = swapped(jnp.concatenate([sums, keep], axis=0), "zh")
    sums = sums + other[: sums.shape[0]]
    keep = in_order(keep, other[sums.shape[0] :], first_side, 0).reshape(2 * share, units)
    gate_value, up_value, grad_hidden = jnp.split(sums, 3, axis=0)

    keep_factor = keep * keep_scale
    sigmoid_gate = jax.nn.sigmoid(gate_value)
    silu_gate = gate_value * sigmoid_gate
    hidden = silu_gate * up_value * keep_factor
    grad_pre = grad_hidden * keep_factor
    grad_gate = grad_pre * up_value * sigmoid_gate * (1.0 + gate_value * (1.0 - sigmoid_gate))
    grad_up = grad_pre * silu_gate
    mine = jnp.concatenate([hidden, grad_gate, grad_up], axis=0).astype(bf16)
    spread = sent_to_all(mine, "y")

    parts = back_products(spread, weights).reshape(2, chips, 2, -1, lanes)
    kept = jnp.where(first_core, parts[:, :, 0], parts[:, :, 1])
    given = jnp.where(first_core, parts[:, :, 1], parts[:, :, 0])
    other = swapped(given, "core")
    down_grad, gate_grad, up_grad = weight_gradients(spread, all_tokens, all_cot)
    parts = jnp.swapaxes((kept + other).astype(bf16), 0, 1).reshape(chips, -1, lanes)
    mixed_out, input_grad = own_outputs(exchange(parts, plane), own, width)
    return (mixed_out, input_grad, gate_grad, up_grad, down_grad)


def solution(mesh):
    fine = Mesh(mesh.devices.reshape(4, 4, 2, 8, 2), ("x", "zl", "core", "y", "zh"))
    row, col = ("x", "zl", "core"), ("y", "zh")
    by_row, by_col = P(row, col), P(col, row)

    return jax.shard_map(
        body,
        mesh=fine,
        in_specs=(by_row, by_col, by_col, by_row, by_col, by_row),
        out_specs=(by_row, by_row, by_col, by_col, by_row),
        check_vma=False,
    )
```

```python
import jax
import jax.numpy as jnp
from jax import lax
from jax.experimental import pallas as pl
from jax.experimental.pallas import tpu as pltpu
from jax.sharding import Mesh
from jax.sharding import PartitionSpec as P

keep_scale = 1.0 / 0.9
contract_last = (((1,), (1,)), ((), ()))
contract_first = (((0,), (0,)), ((), ()))
lanes = 128
plane = ("x", "zl")


def exchange(blocks, axis):
    return lax.all_to_all(blocks, axis, split_axis=0, concat_axis=0, tiled=True)


def sent_to_all(block, axis):
    copies = jnp.broadcast_to(block, (lax.axis_size(axis), *block.shape))
    return exchange(copies, axis)


def swapped(value, axis):
    return lax.ppermute(value, axis, [(0, 1), (1, 0)])


def in_order(mine, other, first, dim):
    a, b = jnp.where(first, mine, other), jnp.where(first, other, mine)
    return jnp.stack([a, b], axis=dim)


def dot(a, b, dims=(((1,), (0,)), ((), ()))):
    return lax.dot_general(a, b, dims, preferred_element_type=jnp.float32)


def vmem_call(kernel, operands, outs, flops, scratch=(), limit=8 << 20, out_space=pltpu.VMEM):
    space, to = (pl.BlockSpec(memory_space=m) for m in (pltpu.VMEM, out_space))
    read = 4 * sum(a.size for a in operands)
    operands = [pltpu.with_memory_space_constraint(a, pltpu.VMEM) for a in operands]
    return pl.pallas_call(
        kernel,
        out_shape=tuple(out_space(*o) for o in outs),
        in_specs=[space] * len(operands),
        out_specs=(to,) * len(outs),
        scratch_shapes=scratch,
        cost_estimate=pl.CostEstimate(flops=flops, bytes_accessed=read, transcendentals=0),
        compiler_params=pltpu.CompilerParams(vmem_limit_bytes=limit),
    )(*operands)


def read_weights(near, weights, keep_mask):
    def kernel(n_ref, g_hbm, u_hbm, d_hbm, k_hbm, g_ref, u_ref, d_ref, keep_ref, mask, sems):
        pairs = ((g_hbm, g_ref), (u_hbm, u_ref), (d_hbm, d_ref), (k_hbm, mask))
        moves = [pltpu.make_async_copy(*pair, sems.at[i]) for i, pair in enumerate(pairs)]
        for move in moves:
            move.start()
        moves[3].wait()
        keep_ref[...] = mask[...].astype(keep_ref.dtype)
        for move in moves[:3]:
            move.wait()

    space, far = (pl.BlockSpec(memory_space=m) for m in (pltpu.VMEM, pltpu.HBM))
    operands = [pltpu.with_memory_space_constraint(a, pltpu.HBM) for a in (*weights, keep_mask)]
    return pl.pallas_call(
        kernel,
        out_shape=(
            *(pltpu.VMEM(w.shape, w.dtype) for w in weights),
            pltpu.VMEM(keep_mask.shape, jnp.bfloat16),
        ),
        in_specs=[space, far, far, far, far],
        out_specs=(space,) * 4,
        scratch_shapes=[
            pltpu.VMEM(keep_mask.shape, keep_mask.dtype),
            pltpu.SemaphoreType.DMA((4,)),
        ],
        cost_estimate=pl.CostEstimate(flops=10**9, bytes_accessed=2 << 20, transcendentals=0),
        compiler_params=pltpu.CompilerParams(vmem_limit_bytes=4 << 20),
        name="read_weights",
    )(near, *operands)


def back_products(spread, weights):
    _, _, down_weight = weights
    ring, rows, units = spread.shape
    rows = rows // 3
    total, width = ring * rows, down_weight.shape[1]

    def kernel(s_ref, g_ref, u_ref, d_ref, out_ref):
        hidden, gate, up = (
            s_ref[:, m * rows : (m + 1) * rows, :].reshape(total, units) for m in range(3)
        )
        out_ref[0] = dot(hidden, d_ref[...])
        out_ref[1] = dot(gate, g_ref[...], contract_last) + dot(up, u_ref[...], contract_last)

    outs = (((2, total, width), jnp.float32),)
    flops = 6 * total * width * units
    return vmem_call(kernel, (spread, *weights), outs, flops)[0]


def weight_gradients(spread, tokens, cotangent):
    _, rows, units = spread.shape
    rows = rows // 3
    total, width = tokens.shape

    def kernel(s_ref, t_ref, c_ref, down_hbm, gate_hbm, up_hbm, down_ref, gate_ref, up_ref, sems):
        hidden, gate, up = (
            s_ref[:, m * rows : (m + 1) * rows, :].reshape(total, units) for m in range(3)
        )
        jobs = (
            (gate_ref, gate_hbm, t_ref, gate),
            (up_ref, up_hbm, t_ref, up),
            (down_ref, down_hbm, None, None),
        )
        moves = []
        for i, (ref, hbm, x_ref, y) in enumerate(jobs):
            x, y = (hidden, c_ref[...]) if x_ref is None else (x_ref[...], y)
            ref[...] = dot(x, y, contract_first).astype(ref.dtype)
            moves.append(pltpu.make_async_copy(ref, hbm, sems.at[i]))
            moves[i].start()
        for move in moves:
            move.wait()

    kind = tokens.dtype
    outs = (((units, width), kind), ((width, units), kind), ((width, units), kind))
    scratch = [*(pltpu.VMEM(*o) for o in outs), pltpu.SemaphoreType.DMA((3,))]
    flops = 6 * total * width * units
    return vmem_call(kernel, (spread, tokens, cotangent), outs, flops, scratch, out_space=pltpu.HBM)


def own_outputs(arrived, own, width):
    def kernel(a_ref, out_ref, in_ref, flat):
        flat[...] = a_ref[...].astype(jnp.float32).sum(axis=0)
        for ref, start in ((out_ref, 0), (in_ref, flat.shape[0] // 2)):
            for c in range(width // lanes):
                piece = flat[pl.ds(start + c, own, stride=width // lanes), :]
                ref[:, c * lanes : (c + 1) * lanes] = piece.astype(ref.dtype)

    space = pl.BlockSpec(memory_space=pltpu.VMEM)
    out = jax.ShapeDtypeStruct((own, width), arrived.dtype)
    return pl.pallas_call(
        kernel,
        out_shape=(out, out),
        in_specs=[space],
        out_specs=(space, space),
        scratch_shapes=[pltpu.VMEM(arrived.shape[1:], jnp.float32)],
        compiler_params=pltpu.CompilerParams(vmem_limit_bytes=4 << 20),
        name="own_outputs",
    )(pltpu.with_memory_space_constraint(arrived, pltpu.VMEM))


def products(tokens, cotangent, weights, place, ring):
    total, units = tokens.shape[0], weights[0].shape[1]
    rows = total // ring

    def kernel(at_ref, t_ref, c_ref, g_ref, u_ref, d_ref, out_ref, lost_ref, whole):
        own = pl.ds(pl.multiple_of(at_ref[0] * rows, rows), rows)

        def put(m, value):
            to = slice(m * rows, (m + 1) * rows)
            out_ref[:, to, :] = value.astype(out_ref.dtype).reshape(ring, rows, units)
            whole[...] = value
            kept = whole[own, :]
            lost_ref[to, :] = kept - kept.astype(out_ref.dtype).astype(jnp.float32)

        put(0, dot(t_ref[...], g_ref[...]))
        put(1, dot(t_ref[...], u_ref[...]))
        put(2, dot(c_ref[...], d_ref[...], contract_last))

    space, smem = (pl.BlockSpec(memory_space=m) for m in (pltpu.VMEM, pltpu.SMEM))
    operands = (tokens, cotangent, *weights)
    operands = [pltpu.with_memory_space_constraint(a, pltpu.VMEM) for a in operands]
    return pl.pallas_call(
        kernel,
        out_shape=(
            pltpu.VMEM((ring, 3 * rows, units), tokens.dtype),
            pltpu.VMEM((3 * rows, units), jnp.float32),
        ),
        in_specs=[smem] + [space] * len(operands),
        out_specs=(space, space),
        scratch_shapes=[pltpu.VMEM((total, units), jnp.float32)],
        compiler_params=pltpu.CompilerParams(vmem_limit_bytes=8 << 20),
        name="products",
    )(place, *operands)


def body(tokens, gate_weight, up_weight, down_weight, keep_mask, cotangent):
    bf16, f32 = jnp.bfloat16, jnp.float32
    own, width = tokens.shape
    share, units = keep_mask.shape
    ring = lax.axis_size("y")
    total = share * 2 * ring
    chips = total // own // 2

    packed = jnp.concatenate([tokens, cotangent], axis=0).reshape(-1, lanes)
    half = packed.shape[0] // 2
    first_core, first_side = lax.axis_index("core") == 0, lax.axis_index("zh") == 0
    place = lax.axis_index("y").reshape(1)
    packed, first_core, first_side, place = lax.optimization_barrier(
        (packed, first_core, first_side, place)
    )
    near = sent_to_all(packed, plane)
    weights = (gate_weight, up_weight, down_weight)
    other = swapped(near, "core")
    *weights, keep = read_weights(near[0, :8], weights, keep_mask)
    both = in_order(near, other, first_core, 1)
    all_tokens = both[:, :, :half].reshape(total, width)
    all_cot = both[:, :, half:].reshape(total, width)

    parts, lost = products(all_tokens, all_cot, weights, place, ring)
    sums = exchange(parts, "y").astype(f32).sum(axis=0) + lost
    high = lax.reduce_precision(sums, 8, 7)
    rows = 2 * share
    low = sums[:rows] - high[:rows]
    other = swapped(jnp.concatenate([high.astype(bf16), low.astype(bf16), keep], axis=0), "zh")
    keep = in_order(keep, other[4 * rows :], first_side, 0).reshape(rows, units).astype(f32)
    other = other[: 4 * rows].astype(f32)
    low = jnp.concatenate([other[3 * rows :], jnp.zeros_like(sums[rows:])], axis=0)
    sums = sums + (other[: 3 * rows] + low)
    gate_value, up_value, grad_hidden = jnp.split(sums, 3, axis=0)

    keep_factor = keep * keep_scale
    sigmoid_gate = jax.nn.sigmoid(gate_value)
    silu_gate = gate_value * sigmoid_gate
    hidden = silu_gate * up_value * keep_factor
    grad_pre = grad_hidden * keep_factor
    grad_gate = grad_pre * up_value * sigmoid_gate * (1.0 + gate_value * (1.0 - sigmoid_gate))
    grad_up = grad_pre * silu_gate
    mine = jnp.concatenate([hidden, grad_gate, grad_up], axis=0).astype(bf16)
    spread = sent_to_all(mine, "y")

    parts = back_products(spread, weights).reshape(2, chips, 2, -1, lanes)
    kept = jnp.where(first_core, parts[:, :, 0], parts[:, :, 1])
    given = jnp.where(first_core, parts[:, :, 1], parts[:, :, 0])
    other = swapped(given, "core")
    down_grad, gate_grad, up_grad = weight_gradients(spread, all_tokens, all_cot)
    parts = jnp.swapaxes((kept + other).astype(bf16), 0, 1).reshape(chips, -1, lanes)
    mixed_out, input_grad = own_outputs(exchange(parts, plane), own, width)
    return (mixed_out, input_grad, gate_grad, up_grad, down_grad)


def solution(mesh):
    fine = Mesh(mesh.devices.reshape(4, 4, 2, 8, 2), ("x", "zl", "core", "y", "zh"))
    row, col = ("x", "zl", "core"), ("y", "zh")
    by_row, by_col = P(row, col), P(col, row)

    return jax.shard_map(
        body,
        mesh=fine,
        in_specs=(by_row, by_col, by_col, by_row, by_col, by_row),
        out_specs=(by_row, by_row, by_col, by_col, by_row),
        check_vma=False,
    )
```

```python
import jax
import jax.numpy as jnp
from jax import lax
from jax.experimental import pallas as pl
from jax.experimental.pallas import tpu as pltpu
from jax.sharding import Mesh
from jax.sharding import PartitionSpec as P

keep_scale = 1.0 / 0.9
contract_last = (((1,), (1,)), ((), ()))
contract_first = (((0,), (0,)), ((), ()))
lanes = 128
plane = ("x", "zl")


def exchange(blocks, axis):
    return lax.all_to_all(blocks, axis, split_axis=0, concat_axis=0, tiled=True)


def sent_to_all(block, axis):
    copies = jnp.broadcast_to(block, (lax.axis_size(axis), *block.shape))
    return exchange(copies, axis)


def swapped(value, axis):
    return lax.ppermute(value, axis, [(0, 1), (1, 0)])


def in_order(mine, other, first, dim):
    a, b = jnp.where(first, mine, other), jnp.where(first, other, mine)
    return jnp.stack([a, b], axis=dim)


def dot(a, b, dims=(((1,), (0,)), ((), ()))):
    return lax.dot_general(a, b, dims, preferred_element_type=jnp.float32)


def vmem_call(kernel, operands, outs, flops, scratch=(), limit=8 << 20, out_space=pltpu.VMEM):
    space, to = (pl.BlockSpec(memory_space=m) for m in (pltpu.VMEM, out_space))
    read = 4 * sum(a.size for a in operands)
    operands = [pltpu.with_memory_space_constraint(a, pltpu.VMEM) for a in operands]
    return pl.pallas_call(
        kernel,
        out_shape=tuple(out_space(*o) for o in outs),
        in_specs=[space] * len(operands),
        out_specs=(to,) * len(outs),
        scratch_shapes=scratch,
        cost_estimate=pl.CostEstimate(flops=flops, bytes_accessed=read, transcendentals=0),
        compiler_params=pltpu.CompilerParams(vmem_limit_bytes=limit),
    )(*operands)


def read_weights(near, weights, keep_mask):
    def kernel(n_ref, g_hbm, u_hbm, d_hbm, k_hbm, g_ref, u_ref, d_ref, keep_ref, mask, sems):
        pairs = ((g_hbm, g_ref), (u_hbm, u_ref), (d_hbm, d_ref), (k_hbm, mask))
        moves = [pltpu.make_async_copy(*pair, sems.at[i]) for i, pair in enumerate(pairs)]
        for move in moves:
            move.start()
        moves[3].wait()
        keep_ref[...] = mask[...].astype(keep_ref.dtype)
        for move in moves[:3]:
            move.wait()

    space, far = (pl.BlockSpec(memory_space=m) for m in (pltpu.VMEM, pltpu.HBM))
    operands = [pltpu.with_memory_space_constraint(a, pltpu.HBM) for a in (*weights, keep_mask)]
    return pl.pallas_call(
        kernel,
        out_shape=(
            *(pltpu.VMEM(w.shape, w.dtype) for w in weights),
            pltpu.VMEM(keep_mask.shape, jnp.bfloat16),
        ),
        in_specs=[space, far, far, far, far],
        out_specs=(space,) * 4,
        scratch_shapes=[
            pltpu.VMEM(keep_mask.shape, keep_mask.dtype),
            pltpu.SemaphoreType.DMA((4,)),
        ],
        cost_estimate=pl.CostEstimate(flops=10**9, bytes_accessed=2 << 20, transcendentals=0),
        compiler_params=pltpu.CompilerParams(vmem_limit_bytes=4 << 20),
        name="read_weights",
    )(near, *operands)


def back_products(spread, weights):
    _, _, down_weight = weights
    ring, rows, units = spread.shape
    rows = rows // 3
    total, width = ring * rows, down_weight.shape[1]

    def kernel(s_ref, g_ref, u_ref, d_ref, out_ref):
        hidden, gate, up = (
            s_ref[:, m * rows : (m + 1) * rows, :].reshape(total, units) for m in range(3)
        )
        out_ref[0] = dot(hidden, d_ref[...])
        out_ref[1] = dot(gate, g_ref[...], contract_last) + dot(up, u_ref[...], contract_last)

    outs = (((2, total, width), jnp.float32),)
    flops = 6 * total * width * units
    return vmem_call(kernel, (spread, *weights), outs, flops)[0]


def weight_gradients(spread, tokens, cotangent):
    _, rows, units = spread.shape
    rows = rows // 3
    total, width = tokens.shape

    def kernel(s_ref, t_ref, c_ref, down_hbm, gate_hbm, up_hbm, down_ref, gate_ref, up_ref, sems):
        hidden, gate, up = (
            s_ref[:, m * rows : (m + 1) * rows, :].reshape(total, units) for m in range(3)
        )
        jobs = (
            (gate_ref, gate_hbm, t_ref, gate),
            (up_ref, up_hbm, t_ref, up),
            (down_ref, down_hbm, None, None),
        )
        moves = []
        for i, (ref, hbm, x_ref, y) in enumerate(jobs):
            x, y = (hidden, c_ref[...]) if x_ref is None else (x_ref[...], y)
            ref[...] = dot(x, y, contract_first).astype(ref.dtype)
            moves.append(pltpu.make_async_copy(ref, hbm, sems.at[i]))
            moves[i].start()
        for move in moves:
            move.wait()

    kind = tokens.dtype
    outs = (((units, width), kind), ((width, units), kind), ((width, units), kind))
    scratch = [*(pltpu.VMEM(*o) for o in outs), pltpu.SemaphoreType.DMA((3,))]
    flops = 6 * total * width * units
    return vmem_call(kernel, (spread, tokens, cotangent), outs, flops, scratch, out_space=pltpu.HBM)


def own_outputs(arrived, own, width):
    def kernel(a_ref, out_ref, in_ref, flat):
        flat[...] = a_ref[...].astype(jnp.float32).sum(axis=0)
        for ref, start in ((out_ref, 0), (in_ref, flat.shape[0] // 2)):
            for c in range(width // lanes):
                piece = flat[pl.ds(start + c, own, stride=width // lanes), :]
                ref[:, c * lanes : (c + 1) * lanes] = piece.astype(ref.dtype)

    space = pl.BlockSpec(memory_space=pltpu.VMEM)
    out = jax.ShapeDtypeStruct((own, width), arrived.dtype)
    return pl.pallas_call(
        kernel,
        out_shape=(out, out),
        in_specs=[space],
        out_specs=(space, space),
        scratch_shapes=[pltpu.VMEM(arrived.shape[1:], jnp.float32)],
        compiler_params=pltpu.CompilerParams(vmem_limit_bytes=4 << 20),
        name="own_outputs",
    )(pltpu.with_memory_space_constraint(arrived, pltpu.VMEM))


def products(tokens, cotangent, weights, place, ring):
    total, units = tokens.shape[0], weights[0].shape[1]
    rows = total // ring

    def kernel(at_ref, t_ref, c_ref, g_ref, u_ref, d_ref, out_ref, lost_ref, whole):
        own = pl.ds(pl.multiple_of(at_ref[0] * rows, rows), rows)

        def put(m, value):
            to = slice(m * rows, (m + 1) * rows)
            out_ref[:, to, :] = value.astype(out_ref.dtype).reshape(ring, rows, units)
            whole[...] = value
            kept = whole[own, :]
            lost_ref[to, :] = kept - kept.astype(out_ref.dtype).astype(jnp.float32)

        put(0, dot(t_ref[...], g_ref[...]))
        put(1, dot(t_ref[...], u_ref[...]))
        put(2, dot(c_ref[...], d_ref[...], contract_last))

    space, smem = (pl.BlockSpec(memory_space=m) for m in (pltpu.VMEM, pltpu.SMEM))
    operands = (tokens, cotangent, *weights)
    operands = [pltpu.with_memory_space_constraint(a, pltpu.VMEM) for a in operands]
    return pl.pallas_call(
        kernel,
        out_shape=(
            pltpu.VMEM((ring, 3 * rows, units), tokens.dtype),
            pltpu.VMEM((3 * rows, units), jnp.float32),
        ),
        in_specs=[smem] + [space] * len(operands),
        out_specs=(space, space),
        scratch_shapes=[pltpu.VMEM((total, units), jnp.float32)],
        compiler_params=pltpu.CompilerParams(vmem_limit_bytes=8 << 20),
        name="products",
    )(place, *operands)


def body(tokens, gate_weight, up_weight, down_weight, keep_mask, cotangent):
    bf16, f32 = jnp.bfloat16, jnp.float32
    own, width = tokens.shape
    share, units = keep_mask.shape
    ring = lax.axis_size("y")
    total = share * 2 * ring
    chips = total // own // 2

    packed = jnp.concatenate([tokens, cotangent], axis=0).reshape(-1, lanes)
    half = packed.shape[0] // 2
    first_core, first_side = lax.axis_index("core") == 0, lax.axis_index("zh") == 0
    place = lax.axis_index("y").reshape(1)
    packed, first_core, first_side, place = lax.optimization_barrier(
        (packed, first_core, first_side, place)
    )
    near = sent_to_all(packed, plane)
    weights = (gate_weight, up_weight, down_weight)
    other = swapped(near, "core")
    *weights, keep = read_weights(near[0, :8], weights, keep_mask)
    both = in_order(near, other, first_core, 1)
    all_tokens = both[:, :, :half].reshape(total, width)
    all_cot = both[:, :, half:].reshape(total, width)

    parts, lost = products(all_tokens, all_cot, weights, place, ring)
    sums = exchange(parts, "y").astype(f32).sum(axis=0) + lost
    rows = 2 * share
    other = swapped(jnp.concatenate([sums.astype(bf16), keep], axis=0), "zh")
    keep = in_order(keep, other[3 * rows :], first_side, 0).reshape(rows, units).astype(f32)
    sums = sums + other[: 3 * rows].astype(f32)
    gate_value, up_value, grad_hidden = jnp.split(sums, 3, axis=0)

    keep_factor = keep * keep_scale
    sigmoid_gate = jax.nn.sigmoid(gate_value)
    silu_gate = gate_value * sigmoid_gate
    hidden = silu_gate * up_value * keep_factor
    grad_pre = grad_hidden * keep_factor
    grad_gate = grad_pre * up_value * sigmoid_gate * (1.0 + gate_value * (1.0 - sigmoid_gate))
    grad_up = grad_pre * silu_gate
    mine = jnp.concatenate([hidden, grad_gate, grad_up], axis=0).astype(bf16)
    spread = sent_to_all(mine, "y")

    parts = back_products(spread, weights).reshape(2, chips, 2, -1, lanes)
    kept = jnp.where(first_core, parts[:, :, 0], parts[:, :, 1])
    given = jnp.where(first_core, parts[:, :, 1], parts[:, :, 0])
    other = swapped(given, "core")
    down_grad, gate_grad, up_grad = weight_gradients(spread, all_tokens, all_cot)
    parts = jnp.swapaxes((kept + other).astype(bf16), 0, 1).reshape(chips, -1, lanes)
    mixed_out, input_grad = own_outputs(exchange(parts, plane), own, width)
    return (mixed_out, input_grad, gate_grad, up_grad, down_grad)


def solution(mesh):
    fine = Mesh(mesh.devices.reshape(4, 4, 2, 8, 2), ("x", "zl", "core", "y", "zh"))
    row, col = ("x", "zl", "core"), ("y", "zh")
    by_row, by_col = P(row, col), P(col, row)

    return jax.shard_map(
        body,
        mesh=fine,
        in_specs=(by_row, by_col, by_col, by_row, by_col, by_row),
        out_specs=(by_row, by_row, by_col, by_col, by_row),
        check_vma=False,
    )
```

```python
import jax
import jax.numpy as jnp
from jax import lax
from jax.experimental import pallas as pl
from jax.experimental.pallas import tpu as pltpu
from jax.sharding import Mesh
from jax.sharding import PartitionSpec as P

keep_scale = 1.0 / 0.9
contract_last = (((1,), (1,)), ((), ()))
contract_first = (((0,), (0,)), ((), ()))
lanes = 128
plane = ("x", "zl")


def exchange(blocks, axis):
    return lax.all_to_all(blocks, axis, split_axis=0, concat_axis=0, tiled=True)


def sent_to_all(block, axis):
    copies = jnp.broadcast_to(block, (lax.axis_size(axis), *block.shape))
    return exchange(copies, axis)


def swapped(value, axis):
    return lax.ppermute(value, axis, [(0, 1), (1, 0)])


def dot(a, b, dims=(((1,), (0,)), ((), ()))):
    return lax.dot_general(a, b, dims, preferred_element_type=jnp.float32)


def vmem_call(kernel, operands, outs, flops, scratch=(), limit=8 << 20, out_space=pltpu.VMEM):
    space, to = (pl.BlockSpec(memory_space=m) for m in (pltpu.VMEM, out_space))
    read = 4 * sum(a.size for a in operands)
    operands = [pltpu.with_memory_space_constraint(a, pltpu.VMEM) for a in operands]
    return pl.pallas_call(
        kernel,
        out_shape=tuple(out_space(*o) for o in outs),
        in_specs=[space] * len(operands),
        out_specs=(to,) * len(outs),
        scratch_shapes=scratch,
        cost_estimate=pl.CostEstimate(flops=flops, bytes_accessed=read, transcendentals=0),
        compiler_params=pltpu.CompilerParams(vmem_limit_bytes=limit),
    )(*operands)


def read_weights(core, near, weights, keep_mask):
    half = keep_mask.shape[0] // 2

    def kernel(
        core_ref, n_ref, g_hbm, u_hbm, d_hbm, k_hbm,
        g_ref, u_ref, d_ref, keep_ref, mask, ordered, sems,
    ):
        pairs = ((g_hbm, g_ref), (u_hbm, u_ref), (d_hbm, d_ref), (k_hbm, mask))
        moves = [pltpu.make_async_copy(*pair, sems.at[i]) for i, pair in enumerate(pairs)]
        for move in moves:
            move.start()
        moves[3].wait()
        whole = mask[...].astype(jnp.float32)
        a, b, first = whole[:half], whole[half:], core_ref[0] == 0
        ordered[:half, :] = jnp.where(first, a, b)
        ordered[half:, :] = jnp.where(first, b, a)
        keep_ref[...] = ordered[...].astype(keep_ref.dtype)
        for move in moves[:3]:
            move.wait()

    space, far = (pl.BlockSpec(memory_space=m) for m in (pltpu.VMEM, pltpu.HBM))
    operands = [pltpu.with_memory_space_constraint(a, pltpu.HBM) for a in (*weights, keep_mask)]
    return pl.pallas_call(
        kernel,
        out_shape=(
            *(pltpu.VMEM(w.shape, w.dtype) for w in weights),
            pltpu.VMEM(keep_mask.shape, jnp.bfloat16),
        ),
        in_specs=[pl.BlockSpec(memory_space=pltpu.SMEM), space, far, far, far, far],
        out_specs=(space,) * 4,
        scratch_shapes=[
            pltpu.VMEM(keep_mask.shape, keep_mask.dtype),
            pltpu.VMEM(keep_mask.shape, jnp.float32),
            pltpu.SemaphoreType.DMA((4,)),
        ],
        cost_estimate=pl.CostEstimate(flops=10**9, bytes_accessed=2 << 20, transcendentals=0),
        compiler_params=pltpu.CompilerParams(vmem_limit_bytes=4 << 20),
        name="read_weights",
    )(core, near, *operands)


def activations(side, sums, other, keep, ring):
    rows, units = sums.shape
    rows = rows // 3
    half = rows // 2

    def kernel(side_ref, s_ref, o_ref, k_ref, out_ref, factor):
        mine = k_ref[...].astype(jnp.float32)
        far = o_ref[3 * rows :, :].astype(jnp.float32)
        first = side_ref[0] == 0
        factor[:half, :] = jnp.where(first, mine, far)
        factor[half:, :] = jnp.where(first, far, mine)
        cuts = [slice(m * rows, (m + 1) * rows) for m in range(3)]
        gate, up, grad = (s_ref[c, :] + o_ref[c, :].astype(jnp.float32) for c in cuts)
        keep_factor = factor[...] * keep_scale
        sigmoid_gate = jax.nn.sigmoid(gate)
        silu_gate = gate * sigmoid_gate
        grad_pre = grad * keep_factor
        values = (
            silu_gate * up * keep_factor,
            grad_pre * up * sigmoid_gate * (1.0 + gate * (1.0 - sigmoid_gate)),
            grad_pre * silu_gate,
        )
        for cut, value in zip(cuts, values):
            value = value.astype(out_ref.dtype)
            for y in range(ring):
                out_ref[y, cut, :] = value

    space, smem = (pl.BlockSpec(memory_space=m) for m in (pltpu.VMEM, pltpu.SMEM))
    operands = [pltpu.with_memory_space_constraint(a, pltpu.VMEM) for a in (sums, other, keep)]
    return pl.pallas_call(
        kernel,
        out_shape=pltpu.VMEM((ring, 3 * rows, units), jnp.bfloat16),
        in_specs=[smem, space, space, space],
        out_specs=space,
        scratch_shapes=[pltpu.VMEM((rows, units), jnp.float32)],
        compiler_params=pltpu.CompilerParams(vmem_limit_bytes=4 << 20),
        name="activations",
    )(side, *operands)


def back_products(spread, weights):
    _, _, down_weight = weights
    ring, rows, units = spread.shape
    rows = rows // 3
    total, width = ring * rows, down_weight.shape[1]

    def kernel(s_ref, g_ref, u_ref, d_ref, out_ref):
        hidden, gate, up = (
            s_ref[:, m * rows : (m + 1) * rows, :].reshape(total, units) for m in range(3)
        )
        out_ref[0] = dot(hidden, d_ref[...])
        out_ref[1] = dot(gate, g_ref[...], contract_last) + dot(up, u_ref[...], contract_last)

    outs = (((2, total, width), jnp.float32),)
    flops = 6 * total * width * units
    return vmem_call(kernel, (spread, *weights), outs, flops)[0]


def weight_gradients(spread, tokens, cotangent):
    _, rows, units = spread.shape
    rows = rows // 3
    total, width = tokens.shape

    def kernel(s_ref, t_ref, c_ref, down_hbm, gate_hbm, up_hbm, down_ref, gate_ref, up_ref, sems):
        hidden, gate, up = (
            s_ref[:, m * rows : (m + 1) * rows, :].reshape(total, units) for m in range(3)
        )
        jobs = (
            (gate_ref, gate_hbm, t_ref, gate),
            (up_ref, up_hbm, t_ref, up),
            (down_ref, down_hbm, None, None),
        )
        moves = []
        for i, (ref, hbm, x_ref, y) in enumerate(jobs):
            x, y = (hidden, c_ref[...]) if x_ref is None else (x_ref[...], y)
            ref[...] = dot(x, y, contract_first).astype(ref.dtype)
            moves.append(pltpu.make_async_copy(ref, hbm, sems.at[i]))
            moves[i].start()
        for move in moves:
            move.wait()

    kind = tokens.dtype
    outs = (((units, width), kind), ((width, units), kind), ((width, units), kind))
    scratch = [*(pltpu.VMEM(*o) for o in outs), pltpu.SemaphoreType.DMA((3,))]
    flops = 6 * total * width * units
    return vmem_call(kernel, (spread, tokens, cotangent), outs, flops, scratch, out_space=pltpu.HBM)


def own_outputs(arrived, own, width):
    def kernel(a_ref, out_ref, in_ref, flat):
        flat[...] = a_ref[...].astype(jnp.float32).sum(axis=0)
        for ref, start in ((out_ref, 0), (in_ref, flat.shape[0] // 2)):
            for c in range(width // lanes):
                piece = flat[pl.ds(start + c, own, stride=width // lanes), :]
                ref[:, c * lanes : (c + 1) * lanes] = piece.astype(ref.dtype)

    space = pl.BlockSpec(memory_space=pltpu.VMEM)
    out = jax.ShapeDtypeStruct((own, width), arrived.dtype)
    return pl.pallas_call(
        kernel,
        out_shape=(out, out),
        in_specs=[space],
        out_specs=(space, space),
        scratch_shapes=[pltpu.VMEM(arrived.shape[1:], jnp.float32)],
        compiler_params=pltpu.CompilerParams(vmem_limit_bytes=4 << 20),
        name="own_outputs",
    )(pltpu.with_memory_space_constraint(arrived, pltpu.VMEM))


def products(tokens, cotangent, weights, place, ring):
    total, units = tokens.shape[0], weights[0].shape[1]
    rows = total // ring

    def kernel(at_ref, t_ref, c_ref, g_ref, u_ref, d_ref, out_ref, lost_ref, whole):
        own = pl.ds(pl.multiple_of(at_ref[0] * rows, rows), rows)

        def put(m, value):
            to = slice(m * rows, (m + 1) * rows)
            out_ref[:, to, :] = value.astype(out_ref.dtype).reshape(ring, rows, units)
            whole[...] = value
            kept = whole[own, :]
            lost_ref[to, :] = kept - kept.astype(out_ref.dtype).astype(jnp.float32)

        put(0, dot(t_ref[...], g_ref[...]))
        put(1, dot(t_ref[...], u_ref[...]))
        put(2, dot(c_ref[...], d_ref[...], contract_last))

    space, smem = (pl.BlockSpec(memory_space=m) for m in (pltpu.VMEM, pltpu.SMEM))
    operands = (tokens, cotangent, *weights)
    operands = [pltpu.with_memory_space_constraint(a, pltpu.VMEM) for a in operands]
    return pl.pallas_call(
        kernel,
        out_shape=(
            pltpu.VMEM((ring, 3 * rows, units), tokens.dtype),
            pltpu.VMEM((3 * rows, units), jnp.float32),
        ),
        in_specs=[smem] + [space] * len(operands),
        out_specs=(space, space),
        scratch_shapes=[pltpu.VMEM((total, units), jnp.float32)],
        compiler_params=pltpu.CompilerParams(vmem_limit_bytes=8 << 20),
        name="products",
    )(place, *operands)


def body(tokens, gate_weight, up_weight, down_weight, keep_mask, cotangent):
    bf16, f32 = jnp.bfloat16, jnp.float32
    own, width = tokens.shape
    share, _ = keep_mask.shape
    ring = lax.axis_size("y")
    total = share * 2 * ring
    chips = total // own // 2

    packed = jnp.concatenate([tokens, cotangent], axis=0).reshape(-1, lanes)
    half = packed.shape[0] // 2
    places = tuple(lax.axis_index(axis).reshape(1) for axis in ("core", "zh", "y"))
    packed, core, side, place = lax.optimization_barrier((packed, *places))
    near = sent_to_all(packed, plane)
    weights = (gate_weight, up_weight, down_weight)
    other = swapped(near, "core")
    *weights, keep = read_weights(core, near[0, :8], weights, keep_mask)
    both = jnp.stack([near, other], axis=1)
    all_tokens = both[:, :, :half].reshape(total, width)
    all_cot = both[:, :, half:].reshape(total, width)

    parts, lost = products(all_tokens, all_cot, weights, place, ring)
    sums = exchange(parts, "y").astype(f32).sum(axis=0) + lost
    other = swapped(jnp.concatenate([sums.astype(bf16), keep], axis=0), "zh")
    spread = exchange(activations(side, sums, other, keep, ring), "y")

    parts = back_products(spread, weights).reshape(2, chips, 2, -1, lanes)
    kept, given = parts[:, :, 0], parts[:, :, 1]
    other = swapped(given, "core")
    down_grad, gate_grad, up_grad = weight_gradients(spread, all_tokens, all_cot)
    parts = jnp.swapaxes((kept + other).astype(bf16), 0, 1).reshape(chips, -1, lanes)
    mixed_out, input_grad = own_outputs(exchange(parts, plane), own, width)
    return (mixed_out, input_grad, gate_grad, up_grad, down_grad)


def solution(mesh):
    fine = Mesh(mesh.devices.reshape(4, 4, 2, 8, 2), ("x", "zl", "core", "y", "zh"))
    row, col = ("x", "zl", "core"), ("y", "zh")
    by_row, by_col = P(row, col), P(col, row)

    return jax.shard_map(
        body,
        mesh=fine,
        in_specs=(by_row, by_col, by_col, by_row, by_col, by_row),
        out_specs=(by_row, by_row, by_col, by_col, by_row),
        check_vma=False,
    )
```

```python
import jax
import jax.numpy as jnp
from jax import lax
from jax.experimental import pallas as pl
from jax.experimental.pallas import tpu as pltpu
from jax.sharding import Mesh
from jax.sharding import PartitionSpec as P

keep_scale = 1.0 / 0.9
contract_last = (((1,), (1,)), ((), ()))
contract_first = (((0,), (0,)), ((), ()))
lanes = 128
plane = ("x", "zl")


def exchange(blocks, axis):
    return lax.all_to_all(blocks, axis, split_axis=0, concat_axis=0, tiled=True)


def sent_to_all(block, axis):
    copies = jnp.broadcast_to(block, (lax.axis_size(axis), *block.shape))
    return exchange(copies, axis)


def swapped(value, axis):
    return lax.ppermute(value, axis, [(0, 1), (1, 0)])


def dot(a, b, dims=(((1,), (0,)), ((), ()))):
    return lax.dot_general(a, b, dims, preferred_element_type=jnp.float32)


def vmem_call(kernel, operands, outs, flops, scratch=(), limit=8 << 20, out_space=pltpu.VMEM):
    space, to = (pl.BlockSpec(memory_space=m) for m in (pltpu.VMEM, out_space))
    read = 4 * sum(a.size for a in operands)
    operands = [pltpu.with_memory_space_constraint(a, pltpu.VMEM) for a in operands]
    return pl.pallas_call(
        kernel,
        out_shape=tuple(out_space(*o) for o in outs),
        in_specs=[space] * len(operands),
        out_specs=(to,) * len(outs),
        scratch_shapes=scratch,
        cost_estimate=pl.CostEstimate(flops=flops, bytes_accessed=read, transcendentals=0),
        compiler_params=pltpu.CompilerParams(vmem_limit_bytes=limit),
    )(*operands)


def read_weights(core, near, weights, keep_mask):
    half = keep_mask.shape[0] // 2
    parts = keep_mask.shape[1] // lanes
    packed = (keep_mask.shape[0] * parts, lanes)

    def kernel(
        core_ref, n_ref, g_hbm, u_hbm, d_hbm, k_hbm,
        g_ref, u_ref, d_ref, keep_ref, mask, ordered, sems,
    ):
        pairs = ((g_hbm, g_ref), (u_hbm, u_ref), (d_hbm, d_ref), (k_hbm, mask))
        moves = [pltpu.make_async_copy(*pair, sems.at[i]) for i, pair in enumerate(pairs)]
        for move in moves:
            move.start()
        moves[3].wait()
        whole = mask[...].astype(jnp.float32)
        a, b, first = whole[:half], whole[half:], core_ref[0] == 0
        for c in range(parts):
            to = slice(c * lanes, (c + 1) * lanes)
            at = 2 * half * c
            ordered[at : at + half, :] = jnp.where(first, a, b)[:, to]
            ordered[at + half : at + 2 * half, :] = jnp.where(first, b, a)[:, to]
        keep_ref[...] = ordered[...].astype(keep_ref.dtype)
        for move in moves[:3]:
            move.wait()

    space, far = (pl.BlockSpec(memory_space=m) for m in (pltpu.VMEM, pltpu.HBM))
    operands = [pltpu.with_memory_space_constraint(a, pltpu.HBM) for a in (*weights, keep_mask)]
    return pl.pallas_call(
        kernel,
        out_shape=(
            *(pltpu.VMEM(w.shape, w.dtype) for w in weights),
            pltpu.VMEM(packed, jnp.bfloat16),
        ),
        in_specs=[pl.BlockSpec(memory_space=pltpu.SMEM), space, far, far, far, far],
        out_specs=(space,) * 4,
        scratch_shapes=[
            pltpu.VMEM(keep_mask.shape, keep_mask.dtype),
            pltpu.VMEM(packed, jnp.float32),
            pltpu.SemaphoreType.DMA((4,)),
        ],
        cost_estimate=pl.CostEstimate(flops=10**9, bytes_accessed=2 << 20, transcendentals=0),
        compiler_params=pltpu.CompilerParams(vmem_limit_bytes=4 << 20),
        name="read_weights",
    )(core, near, *operands)


def activations(side, sums, other, keep, ring, parts):
    total = sums.shape[0]
    half = other.shape[0] - total
    rows, half = total // parts // 3, half // parts

    def kernel(side_ref, s_ref, o_ref, k_ref, out_ref, factor):
        mine = k_ref[...].astype(jnp.float32)
        far = o_ref[total:, :].astype(jnp.float32)
        first = side_ref[0] == 0
        near, away = jnp.where(first, mine, far), jnp.where(first, far, mine)
        for c in range(parts):
            factor[:half, :] = near[half * c : half * (c + 1)]
            factor[half:, :] = away[half * c : half * (c + 1)]
            starts = [(3 * c + m) * rows for m in range(3)]
            cuts = [slice(at, at + rows) for at in starts]
            gate, up, grad = (s_ref[cut, :] + o_ref[cut, :].astype(jnp.float32) for cut in cuts)
            keep_factor = factor[...] * keep_scale
            sigmoid_gate = jax.nn.sigmoid(gate)
            silu_gate = gate * sigmoid_gate
            grad_pre = grad * keep_factor
            values = (
                silu_gate * up * keep_factor,
                grad_pre * up * sigmoid_gate * (1.0 + gate * (1.0 - sigmoid_gate)),
                grad_pre * silu_gate,
            )
            for cut, value in zip(cuts, values):
                value = value.astype(out_ref.dtype)
                for y in range(ring):
                    out_ref[y, cut, :] = value

    space, smem = (pl.BlockSpec(memory_space=m) for m in (pltpu.VMEM, pltpu.SMEM))
    operands = [pltpu.with_memory_space_constraint(a, pltpu.VMEM) for a in (sums, other, keep)]
    return pl.pallas_call(
        kernel,
        out_shape=pltpu.VMEM((ring, total, lanes), jnp.bfloat16),
        in_specs=[smem, space, space, space],
        out_specs=space,
        scratch_shapes=[pltpu.VMEM((rows, lanes), jnp.float32)],
        compiler_params=pltpu.CompilerParams(vmem_limit_bytes=4 << 20),
        name="activations",
    )(side, *operands)


def joined(ref, m, rows, parts):
    total = ref.shape[0] * rows
    cuts = [slice((3 * c + m) * rows, (3 * c + m + 1) * rows) for c in range(parts)]
    return jnp.concatenate([ref[:, cut, :].reshape(total, lanes) for cut in cuts], axis=1)


def back_products(spread, weights):
    _, _, down_weight = weights
    units, width = down_weight.shape
    parts = units // lanes
    ring, rows = spread.shape[0], spread.shape[1] // parts // 3
    total = ring * rows

    def kernel(s_ref, g_ref, u_ref, d_ref, out_ref):
        hidden, gate, up = (joined(s_ref, m, rows, parts) for m in range(3))
        out_ref[0] = dot(hidden, d_ref[...])
        out_ref[1] = dot(gate, g_ref[...], contract_last) + dot(up, u_ref[...], contract_last)

    outs = (((2, total, width), jnp.float32),)
    flops = 6 * total * width * units
    return vmem_call(kernel, (spread, *weights), outs, flops)[0]


def weight_gradients(spread, tokens, cotangent):
    total, width = tokens.shape
    ring = spread.shape[0]
    rows = total // ring
    parts = spread.shape[1] // rows // 3
    units = parts * lanes

    def kernel(s_ref, t_ref, c_ref, down_hbm, gate_hbm, up_hbm, down_ref, gate_ref, up_ref, sems):
        hidden, gate, up = (joined(s_ref, m, rows, parts) for m in range(3))
        jobs = (
            (gate_ref, gate_hbm, t_ref, gate),
            (up_ref, up_hbm, t_ref, up),
            (down_ref, down_hbm, None, None),
        )
        moves = []
        for i, (ref, hbm, x_ref, y) in enumerate(jobs):
            x, y = (hidden, c_ref[...]) if x_ref is None else (x_ref[...], y)
            ref[...] = dot(x, y, contract_first).astype(ref.dtype)
            moves.append(pltpu.make_async_copy(ref, hbm, sems.at[i]))
            moves[i].start()
        for move in moves:
            move.wait()

    kind = tokens.dtype
    outs = (((units, width), kind), ((width, units), kind), ((width, units), kind))
    scratch = [*(pltpu.VMEM(*o) for o in outs), pltpu.SemaphoreType.DMA((3,))]
    flops = 6 * total * width * units
    return vmem_call(kernel, (spread, tokens, cotangent), outs, flops, scratch, out_space=pltpu.HBM)


def own_outputs(arrived, own, width):
    def kernel(a_ref, out_ref, in_ref, flat):
        flat[...] = a_ref[...].astype(jnp.float32).sum(axis=0)
        for ref, start in ((out_ref, 0), (in_ref, flat.shape[0] // 2)):
            for c in range(width // lanes):
                piece = flat[pl.ds(start + c, own, stride=width // lanes), :]
                ref[:, c * lanes : (c + 1) * lanes] = piece.astype(ref.dtype)

    space = pl.BlockSpec(memory_space=pltpu.VMEM)
    out = jax.ShapeDtypeStruct((own, width), arrived.dtype)
    return pl.pallas_call(
        kernel,
        out_shape=(out, out),
        in_specs=[space],
        out_specs=(space, space),
        scratch_shapes=[pltpu.VMEM(arrived.shape[1:], jnp.float32)],
        compiler_params=pltpu.CompilerParams(vmem_limit_bytes=4 << 20),
        name="own_outputs",
    )(pltpu.with_memory_space_constraint(arrived, pltpu.VMEM))


def products(tokens, cotangent, weights, place, ring):
    total, units = tokens.shape[0], weights[0].shape[1]
    rows, parts = total // ring, units // lanes

    def kernel(at_ref, t_ref, c_ref, g_ref, u_ref, d_ref, out_ref, lost_ref, whole):
        own = pl.ds(pl.multiple_of(at_ref[0] * rows, rows), rows)

        def put(m, value):
            whole[...] = value
            kept = whole[own, :]
            lost = kept - kept.astype(out_ref.dtype).astype(jnp.float32)
            value = value.astype(out_ref.dtype).reshape(ring, rows, units)
            for c in range(parts):
                to = slice((3 * c + m) * rows, (3 * c + m + 1) * rows)
                out_ref[:, to, :] = value[:, :, c * lanes : (c + 1) * lanes]
                lost_ref[to, :] = lost[:, c * lanes : (c + 1) * lanes]

        put(0, dot(t_ref[...], g_ref[...]))
        put(1, dot(t_ref[...], u_ref[...]))
        put(2, dot(c_ref[...], d_ref[...], contract_last))

    space, smem = (pl.BlockSpec(memory_space=m) for m in (pltpu.VMEM, pltpu.SMEM))
    operands = (tokens, cotangent, *weights)
    operands = [pltpu.with_memory_space_constraint(a, pltpu.VMEM) for a in operands]
    return pl.pallas_call(
        kernel,
        out_shape=(
            pltpu.VMEM((ring, 3 * rows * parts, lanes), tokens.dtype),
            pltpu.VMEM((3 * rows * parts, lanes), jnp.float32),
        ),
        in_specs=[smem] + [space] * len(operands),
        out_specs=(space, space),
        scratch_shapes=[pltpu.VMEM((total, units), jnp.float32)],
        compiler_params=pltpu.CompilerParams(vmem_limit_bytes=8 << 20),
        name="products",
    )(place, *operands)


def body(tokens, gate_weight, up_weight, down_weight, keep_mask, cotangent):
    bf16, f32 = jnp.bfloat16, jnp.float32
    own, width = tokens.shape
    share, units = keep_mask.shape
    ring = lax.axis_size("y")
    total = share * 2 * ring
    chips = total // own // 2

    packed = jnp.concatenate([tokens, cotangent], axis=0).reshape(-1, lanes)
    half = packed.shape[0] // 2
    places = tuple(lax.axis_index(axis).reshape(1) for axis in ("core", "zh", "y"))
    packed, core, side, place = lax.optimization_barrier((packed, *places))
    near = sent_to_all(packed, plane)
    weights = (gate_weight, up_weight, down_weight)
    other = swapped(near, "core")
    *weights, keep = read_weights(core, near[0, :8], weights, keep_mask)
    both = jnp.stack([near, other], axis=1)
    all_tokens = both[:, :, :half].reshape(total, width)
    all_cot = both[:, :, half:].reshape(total, width)

    parts, lost = products(all_tokens, all_cot, weights, place, ring)
    sums = exchange(parts, "y").astype(f32).sum(axis=0) + lost
    other = swapped(jnp.concatenate([sums.astype(bf16), keep], axis=0), "zh")
    spread = exchange(activations(side, sums, other, keep, ring, units // lanes), "y")

    parts = back_products(spread, weights).reshape(2, chips, 2, -1, lanes)
    kept, given = parts[:, :, 0], parts[:, :, 1]
    other = swapped(given, "core")
    down_grad, gate_grad, up_grad = weight_gradients(spread, all_tokens, all_cot)
    parts = jnp.swapaxes((kept + other).astype(bf16), 0, 1).reshape(chips, -1, lanes)
    mixed_out, input_grad = own_outputs(exchange(parts, plane), own, width)
    return (mixed_out, input_grad, gate_grad, up_grad, down_grad)


def solution(mesh):
    fine = Mesh(mesh.devices.reshape(4, 4, 2, 8, 2), ("x", "zl", "core", "y", "zh"))
    row, col = ("x", "zl", "core"), ("y", "zh")
    by_row, by_col = P(row, col), P(col, row)

    return jax.shard_map(
        body,
        mesh=fine,
        in_specs=(by_row, by_col, by_col, by_row, by_col, by_row),
        out_specs=(by_row, by_row, by_col, by_col, by_row),
        check_vma=False,
    )
```

```python
import jax
import jax.numpy as jnp
from jax import lax
from jax.experimental import pallas as pl
from jax.experimental.pallas import tpu as pltpu
from jax.sharding import Mesh
from jax.sharding import PartitionSpec as P

keep_scale = 1.0 / 0.9
contract_last = (((1,), (1,)), ((), ()))
contract_first = (((0,), (0,)), ((), ()))
lanes = 128
plane = ("x", "zl")


def exchange(blocks, axis):
    return lax.all_to_all(blocks, axis, split_axis=0, concat_axis=0, tiled=True)


def sent_to_all(block, axis):
    copies = jnp.broadcast_to(block, (lax.axis_size(axis), *block.shape))
    return exchange(copies, axis)


def swapped(value, axis):
    return lax.ppermute(value, axis, [(0, 1), (1, 0)])


def dot(a, b, dims=(((1,), (0,)), ((), ()))):
    return lax.dot_general(a, b, dims, preferred_element_type=jnp.float32)


def vmem_call(kernel, operands, outs, flops, scratch=(), limit=8 << 20, out_space=pltpu.VMEM):
    space, to = (pl.BlockSpec(memory_space=m) for m in (pltpu.VMEM, out_space))
    read = 4 * sum(a.size for a in operands)
    operands = [pltpu.with_memory_space_constraint(a, pltpu.VMEM) for a in operands]
    return pl.pallas_call(
        kernel,
        out_shape=tuple(out_space(*o) for o in outs),
        in_specs=[space] * len(operands),
        out_specs=(to,) * len(outs),
        scratch_shapes=scratch,
        cost_estimate=pl.CostEstimate(flops=flops, bytes_accessed=read, transcendentals=0),
        compiler_params=pltpu.CompilerParams(vmem_limit_bytes=limit),
    )(*operands)


def read_weights(core, near, weights, keep_mask):
    half = keep_mask.shape[0] // 2
    parts = keep_mask.shape[1] // lanes
    packed = (keep_mask.shape[0] * parts, lanes)

    def kernel(
        core_ref, n_ref, g_hbm, u_hbm, d_hbm, k_hbm,
        g_ref, u_ref, d_ref, keep_ref, mask, ordered, sems,
    ):
        pairs = ((g_hbm, g_ref), (u_hbm, u_ref), (d_hbm, d_ref), (k_hbm, mask))
        moves = [pltpu.make_async_copy(*pair, sems.at[i]) for i, pair in enumerate(pairs)]
        for move in moves:
            move.start()
        moves[3].wait()
        whole = mask[...].astype(jnp.float32)
        a, b, first = whole[:half], whole[half:], core_ref[0] == 0
        for c in range(parts):
            to = slice(c * lanes, (c + 1) * lanes)
            at = 2 * half * c
            ordered[at : at + half, :] = jnp.where(first, a, b)[:, to]
            ordered[at + half : at + 2 * half, :] = jnp.where(first, b, a)[:, to]
        keep_ref[...] = ordered[...].astype(keep_ref.dtype)
        for move in moves[:3]:
            move.wait()

    space, far = (pl.BlockSpec(memory_space=m) for m in (pltpu.VMEM, pltpu.HBM))
    operands = [pltpu.with_memory_space_constraint(a, pltpu.HBM) for a in (*weights, keep_mask)]
    return pl.pallas_call(
        kernel,
        out_shape=(
            *(pltpu.VMEM(w.shape, w.dtype) for w in weights),
            pltpu.VMEM(packed, jnp.bfloat16),
        ),
        in_specs=[pl.BlockSpec(memory_space=pltpu.SMEM), space, far, far, far, far],
        out_specs=(space,) * 4,
        scratch_shapes=[
            pltpu.VMEM(keep_mask.shape, keep_mask.dtype),
            pltpu.VMEM(packed, jnp.float32),
            pltpu.SemaphoreType.DMA((4,)),
        ],
        cost_estimate=pl.CostEstimate(flops=10**9, bytes_accessed=2 << 20, transcendentals=0),
        compiler_params=pltpu.CompilerParams(vmem_limit_bytes=4 << 20),
        name="read_weights",
    )(core, near, *operands)


def activations(side, sums, other, keep, ring, parts):
    total = sums.shape[0]
    rows = total // parts // 3
    more = total + parts * rows
    half = (other.shape[0] - more) // parts

    def kernel(side_ref, s_ref, o_ref, k_ref, out_ref, factor):
        mine = k_ref[...].astype(jnp.float32)
        far = o_ref[more:, :].astype(jnp.float32)
        first = side_ref[0] == 0
        near, away = jnp.where(first, mine, far), jnp.where(first, far, mine)
        for c in range(parts):
            factor[:half, :] = near[half * c : half * (c + 1)]
            factor[half:, :] = away[half * c : half * (c + 1)]
            starts = [(3 * c + m) * rows for m in range(3)]
            cuts = [slice(at, at + rows) for at in starts]
            gate, up, grad = (s_ref[cut, :] + o_ref[cut, :].astype(jnp.float32) for cut in cuts)
            second = slice(total + c * rows, total + (c + 1) * rows)
            gate = gate + o_ref[second, :].astype(jnp.float32)
            keep_factor = factor[...] * keep_scale
            sigmoid_gate = jax.nn.sigmoid(gate)
            silu_gate = gate * sigmoid_gate
            grad_pre = grad * keep_factor
            values = (
                silu_gate * up * keep_factor,
                grad_pre * up * sigmoid_gate * (1.0 + gate * (1.0 - sigmoid_gate)),
                grad_pre * silu_gate,
            )
            for cut, value in zip(cuts, values):
                value = value.astype(out_ref.dtype)
                for y in range(ring):
                    out_ref[y, cut, :] = value

    space, smem = (pl.BlockSpec(memory_space=m) for m in (pltpu.VMEM, pltpu.SMEM))
    operands = [pltpu.with_memory_space_constraint(a, pltpu.VMEM) for a in (sums, other, keep)]
    return pl.pallas_call(
        kernel,
        out_shape=pltpu.VMEM((ring, total, lanes), jnp.bfloat16),
        in_specs=[smem, space, space, space],
        out_specs=space,
        scratch_shapes=[pltpu.VMEM((rows, lanes), jnp.float32)],
        compiler_params=pltpu.CompilerParams(vmem_limit_bytes=4 << 20),
        name="activations",
    )(side, *operands)


def joined(ref, m, rows, parts):
    total = ref.shape[0] * rows
    cuts = [slice((3 * c + m) * rows, (3 * c + m + 1) * rows) for c in range(parts)]
    return jnp.concatenate([ref[:, cut, :].reshape(total, lanes) for cut in cuts], axis=1)


def back_products(spread, weights):
    _, _, down_weight = weights
    units, width = down_weight.shape
    parts = units // lanes
    ring, rows = spread.shape[0], spread.shape[1] // parts // 3
    total = ring * rows

    def kernel(s_ref, g_ref, u_ref, d_ref, out_ref):
        hidden, gate, up = (joined(s_ref, m, rows, parts) for m in range(3))
        out_ref[0] = dot(hidden, d_ref[...])
        out_ref[1] = dot(gate, g_ref[...], contract_last) + dot(up, u_ref[...], contract_last)

    outs = (((2, total, width), jnp.float32),)
    flops = 6 * total * width * units
    return vmem_call(kernel, (spread, *weights), outs, flops)[0]


def weight_gradients(spread, tokens, cotangent):
    total, width = tokens.shape
    ring = spread.shape[0]
    rows = total // ring
    parts = spread.shape[1] // rows // 3
    units = parts * lanes

    def kernel(s_ref, t_ref, c_ref, down_hbm, gate_hbm, up_hbm, down_ref, gate_ref, up_ref, sems):
        hidden, gate, up = (joined(s_ref, m, rows, parts) for m in range(3))
        jobs = (
            (gate_ref, gate_hbm, t_ref, gate),
            (up_ref, up_hbm, t_ref, up),
            (down_ref, down_hbm, None, None),
        )
        moves = []
        for i, (ref, hbm, x_ref, y) in enumerate(jobs):
            x, y = (hidden, c_ref[...]) if x_ref is None else (x_ref[...], y)
            ref[...] = dot(x, y, contract_first).astype(ref.dtype)
            moves.append(pltpu.make_async_copy(ref, hbm, sems.at[i]))
            moves[i].start()
        for move in moves:
            move.wait()

    kind = tokens.dtype
    outs = (((units, width), kind), ((width, units), kind), ((width, units), kind))
    scratch = [*(pltpu.VMEM(*o) for o in outs), pltpu.SemaphoreType.DMA((3,))]
    flops = 6 * total * width * units
    return vmem_call(kernel, (spread, tokens, cotangent), outs, flops, scratch, out_space=pltpu.HBM)


def own_outputs(arrived, own, width):
    def kernel(a_ref, out_ref, in_ref, flat):
        flat[...] = a_ref[...].astype(jnp.float32).sum(axis=0)
        for ref, start in ((out_ref, 0), (in_ref, flat.shape[0] // 2)):
            for c in range(width // lanes):
                piece = flat[pl.ds(start + c, own, stride=width // lanes), :]
                ref[:, c * lanes : (c + 1) * lanes] = piece.astype(ref.dtype)

    space = pl.BlockSpec(memory_space=pltpu.VMEM)
    out = jax.ShapeDtypeStruct((own, width), arrived.dtype)
    return pl.pallas_call(
        kernel,
        out_shape=(out, out),
        in_specs=[space],
        out_specs=(space, space),
        scratch_shapes=[pltpu.VMEM(arrived.shape[1:], jnp.float32)],
        compiler_params=pltpu.CompilerParams(vmem_limit_bytes=4 << 20),
        name="own_outputs",
    )(pltpu.with_memory_space_constraint(arrived, pltpu.VMEM))


def products(tokens, cotangent, weights, place, ring):
    total, units = tokens.shape[0], weights[0].shape[1]
    rows, parts = total // ring, units // lanes

    def kernel(at_ref, t_ref, c_ref, g_ref, u_ref, d_ref, out_ref, lost_ref, whole):
        own = pl.ds(pl.multiple_of(at_ref[0] * rows, rows), rows)

        def put(m, value):
            whole[...] = value
            kept = whole[own, :]
            lost = kept - kept.astype(out_ref.dtype).astype(jnp.float32)
            value = value.astype(out_ref.dtype).reshape(ring, rows, units)
            for c in range(parts):
                to = slice((3 * c + m) * rows, (3 * c + m + 1) * rows)
                out_ref[:, to, :] = value[:, :, c * lanes : (c + 1) * lanes]
                lost_ref[to, :] = lost[:, c * lanes : (c + 1) * lanes]

        put(0, dot(t_ref[...], g_ref[...]))
        put(1, dot(t_ref[...], u_ref[...]))
        put(2, dot(c_ref[...], d_ref[...], contract_last))

    space, smem = (pl.BlockSpec(memory_space=m) for m in (pltpu.VMEM, pltpu.SMEM))
    operands = (tokens, cotangent, *weights)
    operands = [pltpu.with_memory_space_constraint(a, pltpu.VMEM) for a in operands]
    return pl.pallas_call(
        kernel,
        out_shape=(
            pltpu.VMEM((ring, 3 * rows * parts, lanes), tokens.dtype),
            pltpu.VMEM((3 * rows * parts, lanes), jnp.float32),
        ),
        in_specs=[smem] + [space] * len(operands),
        out_specs=(space, space),
        scratch_shapes=[pltpu.VMEM((total, units), jnp.float32)],
        compiler_params=pltpu.CompilerParams(vmem_limit_bytes=8 << 20),
        name="products",
    )(place, *operands)


def body(tokens, gate_weight, up_weight, down_weight, keep_mask, cotangent):
    bf16, f32 = jnp.bfloat16, jnp.float32
    own, width = tokens.shape
    share, units = keep_mask.shape
    ring = lax.axis_size("y")
    total = share * 2 * ring
    chips = total // own // 2

    packed = jnp.concatenate([tokens, cotangent], axis=0).reshape(-1, lanes)
    half = packed.shape[0] // 2
    places = tuple(lax.axis_index(axis).reshape(1) for axis in ("core", "zh", "y"))
    packed, core, side, place = lax.optimization_barrier((packed, *places))
    near = sent_to_all(packed, plane)
    weights = (gate_weight, up_weight, down_weight)
    other = swapped(near, "core")
    *weights, keep = read_weights(core, near[0, :8], weights, keep_mask)
    both = jnp.stack([near, other], axis=1)
    all_tokens = both[:, :, :half].reshape(total, width)
    all_cot = both[:, :, half:].reshape(total, width)

    parts, lost = products(all_tokens, all_cot, weights, place, ring)
    sums = exchange(parts, "y").astype(f32).sum(axis=0) + lost
    high = lax.reduce_precision(sums, 8, 7)
    low = (sums - high).reshape(units // lanes, 3, -1, lanes)[:, 0].reshape(-1, lanes)
    other = swapped(jnp.concatenate([high.astype(bf16), low.astype(bf16), keep], axis=0), "zh")
    spread = exchange(activations(side, sums, other, keep, ring, units // lanes), "y")

    parts = back_products(spread, weights).reshape(2, chips, 2, -1, lanes)
    kept, given = parts[:, :, 0], parts[:, :, 1]
    other = swapped(given, "core")
    down_grad, gate_grad, up_grad = weight_gradients(spread, all_tokens, all_cot)
    parts = jnp.swapaxes((kept + other).astype(bf16), 0, 1).reshape(chips, -1, lanes)
    mixed_out, input_grad = own_outputs(exchange(parts, plane), own, width)
    return (mixed_out, input_grad, gate_grad, up_grad, down_grad)


def solution(mesh):
    fine = Mesh(mesh.devices.reshape(4, 4, 2, 8, 2), ("x", "zl", "core", "y", "zh"))
    row, col = ("x", "zl", "core"), ("y", "zh")
    by_row, by_col = P(row, col), P(col, row)

    return jax.shard_map(
        body,
        mesh=fine,
        in_specs=(by_row, by_col, by_col, by_row, by_col, by_row),
        out_specs=(by_row, by_row, by_col, by_col, by_row),
        check_vma=False,
    )
```

```python
import jax
import jax.numpy as jnp
from jax import lax
from jax.experimental import pallas as pl
from jax.experimental.pallas import tpu as pltpu
from jax.sharding import Mesh
from jax.sharding import PartitionSpec as P

keep_scale = 1.0 / 0.9
contract_last = (((1,), (1,)), ((), ()))
contract_first = (((0,), (0,)), ((), ()))
lanes = 128
plane = ("zl", "x")


def exchange(blocks, axis):
    return lax.all_to_all(blocks, axis, split_axis=0, concat_axis=0, tiled=True)


def sent_to_all(block, axis):
    copies = jnp.broadcast_to(block, (lax.axis_size(axis), *block.shape))
    return exchange(copies, axis)


def flipped(blocks, first, second):
    sizes = lax.axis_size(first), lax.axis_size(second)
    return jnp.swapaxes(blocks.reshape(*sizes, *blocks.shape[1:]), 0, 1).reshape(blocks.shape)


def swapped(value, axis):
    return lax.ppermute(value, axis, [(0, 1), (1, 0)])


def dot(a, b, dims=(((1,), (0,)), ((), ()))):
    return lax.dot_general(a, b, dims, preferred_element_type=jnp.float32)


def vmem_call(kernel, operands, outs, flops, scratch=(), limit=8 << 20, out_space=pltpu.VMEM):
    space, to = (pl.BlockSpec(memory_space=m) for m in (pltpu.VMEM, out_space))
    read = 4 * sum(a.size for a in operands)
    operands = [pltpu.with_memory_space_constraint(a, pltpu.VMEM) for a in operands]
    return pl.pallas_call(
        kernel,
        out_shape=tuple(out_space(*o) for o in outs),
        in_specs=[space] * len(operands),
        out_specs=(to,) * len(outs),
        scratch_shapes=scratch,
        cost_estimate=pl.CostEstimate(flops=flops, bytes_accessed=read, transcendentals=0),
        compiler_params=pltpu.CompilerParams(vmem_limit_bytes=limit),
    )(*operands)


def read_weights(core, near, weights, keep_mask):
    half = keep_mask.shape[0] // 2
    parts = keep_mask.shape[1] // lanes
    packed = (keep_mask.shape[0] * parts, lanes)

    def kernel(
        core_ref, n_ref, g_hbm, u_hbm, d_hbm, k_hbm,
        g_ref, u_ref, d_ref, keep_ref, mask, ordered, sems,
    ):
        pairs = ((g_hbm, g_ref), (u_hbm, u_ref), (d_hbm, d_ref), (k_hbm, mask))
        moves = [pltpu.make_async_copy(*pair, sems.at[i]) for i, pair in enumerate(pairs)]
        for move in moves:
            move.start()
        moves[3].wait()
        whole = mask[...].astype(jnp.float32)
        a, b, first = whole[:half], whole[half:], core_ref[0] == 0
        for c in range(parts):
            to = slice(c * lanes, (c + 1) * lanes)
            at = 2 * half * c
            ordered[at : at + half, :] = jnp.where(first, a, b)[:, to]
            ordered[at + half : at + 2 * half, :] = jnp.where(first, b, a)[:, to]
        keep_ref[...] = ordered[...].astype(keep_ref.dtype)
        for move in moves[:3]:
            move.wait()

    space, far = (pl.BlockSpec(memory_space=m) for m in (pltpu.VMEM, pltpu.HBM))
    operands = [pltpu.with_memory_space_constraint(a, pltpu.HBM) for a in (*weights, keep_mask)]
    return pl.pallas_call(
        kernel,
        out_shape=(
            *(pltpu.VMEM(w.shape, w.dtype) for w in weights),
            pltpu.VMEM(packed, jnp.bfloat16),
        ),
        in_specs=[pl.BlockSpec(memory_space=pltpu.SMEM), space, far, far, far, far],
        out_specs=(space,) * 4,
        scratch_shapes=[
            pltpu.VMEM(keep_mask.shape, keep_mask.dtype),
            pltpu.VMEM(packed, jnp.float32),
            pltpu.SemaphoreType.DMA((4,)),
        ],
        cost_estimate=pl.CostEstimate(flops=10**9, bytes_accessed=2 << 20, transcendentals=0),
        compiler_params=pltpu.CompilerParams(vmem_limit_bytes=4 << 20),
        name="read_weights",
    )(core, near, *operands)


def activations(side, sums, other, keep, ring, parts):
    total = sums.shape[0]
    half = other.shape[0] - total
    rows, half = total // parts // 3, half // parts

    def kernel(side_ref, s_ref, o_ref, k_ref, out_ref, factor):
        mine = k_ref[...].astype(jnp.float32)
        far = o_ref[total:, :].astype(jnp.float32)
        first = side_ref[0] == 0
        near, away = jnp.where(first, mine, far), jnp.where(first, far, mine)
        for c in range(parts):
            factor[:half, :] = near[half * c : half * (c + 1)]
            factor[half:, :] = away[half * c : half * (c + 1)]
            starts = [(3 * c + m) * rows for m in range(3)]
            cuts = [slice(at, at + rows) for at in starts]
            gate, up, grad = (s_ref[cut, :] + o_ref[cut, :].astype(jnp.float32) for cut in cuts)
            keep_factor = factor[...] * keep_scale
            sigmoid_gate = jax.nn.sigmoid(gate)
            silu_gate = gate * sigmoid_gate
            grad_pre = grad * keep_factor
            values = (
                silu_gate * up * keep_factor,
                grad_pre * up * sigmoid_gate * (1.0 + gate * (1.0 - sigmoid_gate)),
                grad_pre * silu_gate,
            )
            for cut, value in zip(cuts, values):
                value = value.astype(out_ref.dtype)
                for y in range(ring):
                    out_ref[y, cut, :] = value

    space, smem = (pl.BlockSpec(memory_space=m) for m in (pltpu.VMEM, pltpu.SMEM))
    operands = [pltpu.with_memory_space_constraint(a, pltpu.VMEM) for a in (sums, other, keep)]
    return pl.pallas_call(
        kernel,
        out_shape=pltpu.VMEM((ring, total, lanes), jnp.bfloat16),
        in_specs=[smem, space, space, space],
        out_specs=space,
        scratch_shapes=[pltpu.VMEM((rows, lanes), jnp.float32)],
        compiler_params=pltpu.CompilerParams(vmem_limit_bytes=4 << 20),
        name="activations",
    )(side, *operands)


def joined(ref, m, rows, parts):
    total = ref.shape[0] * rows
    cuts = [slice((3 * c + m) * rows, (3 * c + m + 1) * rows) for c in range(parts)]
    return jnp.concatenate([ref[:, cut, :].reshape(total, lanes) for cut in cuts], axis=1)


def back_products(spread, weights):
    _, _, down_weight = weights
    units, width = down_weight.shape
    parts = units // lanes
    ring, rows = spread.shape[0], spread.shape[1] // parts // 3
    total = ring * rows

    def kernel(s_ref, g_ref, u_ref, d_ref, out_ref):
        hidden, gate, up = (joined(s_ref, m, rows, parts) for m in range(3))
        out_ref[0] = dot(hidden, d_ref[...])
        out_ref[1] = dot(gate, g_ref[...], contract_last) + dot(up, u_ref[...], contract_last)

    outs = (((2, total, width), jnp.float32),)
    flops = 6 * total * width * units
    return vmem_call(kernel, (spread, *weights), outs, flops)[0]


def weight_gradients(spread, tokens, cotangent):
    total, width = tokens.shape
    ring = spread.shape[0]
    rows = total // ring
    parts = spread.shape[1] // rows // 3
    units = parts * lanes

    def kernel(s_ref, t_ref, c_ref, down_hbm, gate_hbm, up_hbm, down_ref, gate_ref, up_ref, sems):
        hidden, gate, up = (joined(s_ref, m, rows, parts) for m in range(3))
        jobs = (
            (gate_ref, gate_hbm, t_ref, gate),
            (up_ref, up_hbm, t_ref, up),
            (down_ref, down_hbm, None, None),
        )
        moves = []
        for i, (ref, hbm, x_ref, y) in enumerate(jobs):
            x, y = (hidden, c_ref[...]) if x_ref is None else (x_ref[...], y)
            ref[...] = dot(x, y, contract_first).astype(ref.dtype)
            moves.append(pltpu.make_async_copy(ref, hbm, sems.at[i]))
            moves[i].start()
        for move in moves:
            move.wait()

    kind = tokens.dtype
    outs = (((units, width), kind), ((width, units), kind), ((width, units), kind))
    scratch = [*(pltpu.VMEM(*o) for o in outs), pltpu.SemaphoreType.DMA((3,))]
    flops = 6 * total * width * units
    return vmem_call(kernel, (spread, tokens, cotangent), outs, flops, scratch, out_space=pltpu.HBM)


def own_outputs(arrived, own, width):
    def kernel(a_ref, out_ref, in_ref, flat):
        flat[...] = a_ref[...].astype(jnp.float32).sum(axis=0)
        for ref, start in ((out_ref, 0), (in_ref, flat.shape[0] // 2)):
            for c in range(width // lanes):
                piece = flat[pl.ds(start + c, own, stride=width // lanes), :]
                ref[:, c * lanes : (c + 1) * lanes] = piece.astype(ref.dtype)

    space = pl.BlockSpec(memory_space=pltpu.VMEM)
    out = jax.ShapeDtypeStruct((own, width), arrived.dtype)
    return pl.pallas_call(
        kernel,
        out_shape=(out, out),
        in_specs=[space],
        out_specs=(space, space),
        scratch_shapes=[pltpu.VMEM(arrived.shape[1:], jnp.float32)],
        compiler_params=pltpu.CompilerParams(vmem_limit_bytes=4 << 20),
        name="own_outputs",
    )(pltpu.with_memory_space_constraint(arrived, pltpu.VMEM))


def products(tokens, cotangent, weights, place, ring):
    total, units = tokens.shape[0], weights[0].shape[1]
    rows, parts = total // ring, units // lanes

    def kernel(at_ref, t_ref, c_ref, g_ref, u_ref, d_ref, out_ref, lost_ref, whole):
        own = pl.ds(pl.multiple_of(at_ref[0] * rows, rows), rows)

        def put(m, value):
            whole[...] = value
            kept = whole[own, :]
            lost = kept - kept.astype(out_ref.dtype).astype(jnp.float32)
            value = value.astype(out_ref.dtype).reshape(ring, rows, units)
            for c in range(parts):
                to = slice((3 * c + m) * rows, (3 * c + m + 1) * rows)
                out_ref[:, to, :] = value[:, :, c * lanes : (c + 1) * lanes]
                lost_ref[to, :] = lost[:, c * lanes : (c + 1) * lanes]

        put(0, dot(t_ref[...], g_ref[...]))
        put(1, dot(t_ref[...], u_ref[...]))
        put(2, dot(c_ref[...], d_ref[...], contract_last))

    space, smem = (pl.BlockSpec(memory_space=m) for m in (pltpu.VMEM, pltpu.SMEM))
    operands = (tokens, cotangent, *weights)
    operands = [pltpu.with_memory_space_constraint(a, pltpu.VMEM) for a in operands]
    return pl.pallas_call(
        kernel,
        out_shape=(
            pltpu.VMEM((ring, 3 * rows * parts, lanes), tokens.dtype),
            pltpu.VMEM((3 * rows * parts, lanes), jnp.float32),
        ),
        in_specs=[smem] + [space] * len(operands),
        out_specs=(space, space),
        scratch_shapes=[pltpu.VMEM((total, units), jnp.float32)],
        compiler_params=pltpu.CompilerParams(vmem_limit_bytes=8 << 20),
        name="products",
    )(place, *operands)


def body(tokens, gate_weight, up_weight, down_weight, keep_mask, cotangent):
    bf16, f32 = jnp.bfloat16, jnp.float32
    own, width = tokens.shape
    share, units = keep_mask.shape
    ring = lax.axis_size("y")
    total = share * 2 * ring
    chips = total // own // 2

    packed = jnp.concatenate([tokens, cotangent], axis=0).reshape(-1, lanes)
    half = packed.shape[0] // 2
    places = tuple(lax.axis_index(axis).reshape(1) for axis in ("core", "zh", "y"))
    packed, core, side, place = lax.optimization_barrier((packed, *places))
    near = sent_to_all(packed, plane)
    weights = (gate_weight, up_weight, down_weight)
    other = swapped(near, "core")
    *weights, keep = read_weights(core, near[0, :8], weights, keep_mask)
    both = flipped(jnp.stack([near, other], axis=1), *plane)
    all_tokens = both[:, :, :half].reshape(total, width)
    all_cot = both[:, :, half:].reshape(total, width)

    parts, lost = products(all_tokens, all_cot, weights, place, ring)
    sums = exchange(parts, "y").astype(f32).sum(axis=0) + lost
    other = swapped(jnp.concatenate([sums.astype(bf16), keep], axis=0), "zh")
    spread = exchange(activations(side, sums, other, keep, ring, units // lanes), "y")

    parts = back_products(spread, weights).reshape(2, chips, 2, -1, lanes)
    kept, given = parts[:, :, 0], parts[:, :, 1]
    other = swapped(given, "core")
    down_grad, gate_grad, up_grad = weight_gradients(spread, all_tokens, all_cot)
    parts = jnp.swapaxes((kept + other).astype(bf16), 0, 1).reshape(chips, -1, lanes)
    parts = flipped(parts, *plane[::-1])
    mixed_out, input_grad = own_outputs(exchange(parts, plane), own, width)
    return (mixed_out, input_grad, gate_grad, up_grad, down_grad)


def solution(mesh):
    fine = Mesh(mesh.devices.reshape(4, 4, 2, 8, 2), ("x", "zl", "core", "y", "zh"))
    row, col = ("x", "zl", "core"), ("y", "zh")
    by_row, by_col = P(row, col), P(col, row)

    return jax.shard_map(
        body,
        mesh=fine,
        in_specs=(by_row, by_col, by_col, by_row, by_col, by_row),
        out_specs=(by_row, by_row, by_col, by_col, by_row),
        check_vma=False,
    )
```

```python
import jax
import jax.numpy as jnp
from jax import lax
from jax.experimental import pallas as pl
from jax.experimental.pallas import tpu as pltpu
from jax.sharding import Mesh
from jax.sharding import PartitionSpec as P

keep_scale = 1.0 / 0.9
contract_last = (((1,), (1,)), ((), ()))
contract_first = (((0,), (0,)), ((), ()))
lanes = 128
plane = ("x", "zl")


def exchange(blocks, axis):
    return lax.all_to_all(blocks, axis, split_axis=0, concat_axis=0, tiled=True)


def sent_to_all(block, axis):
    copies = jnp.broadcast_to(block, (lax.axis_size(axis), *block.shape))
    return exchange(copies, axis)


def swapped(value, axis):
    return lax.ppermute(value, axis, [(0, 1), (1, 0)])


def dot(a, b, dims=(((1,), (0,)), ((), ()))):
    return lax.dot_general(a, b, dims, preferred_element_type=jnp.float32)


def vmem_call(kernel, operands, outs, flops, scratch=(), limit=8 << 20, out_space=pltpu.VMEM):
    space, to = (pl.BlockSpec(memory_space=m) for m in (pltpu.VMEM, out_space))
    read = 4 * sum(a.size for a in operands)
    operands = [pltpu.with_memory_space_constraint(a, pltpu.VMEM) for a in operands]
    return pl.pallas_call(
        kernel,
        out_shape=tuple(out_space(*o) for o in outs),
        in_specs=[space] * len(operands),
        out_specs=(to,) * len(outs),
        scratch_shapes=scratch,
        cost_estimate=pl.CostEstimate(flops=flops, bytes_accessed=read, transcendentals=0),
        compiler_params=pltpu.CompilerParams(vmem_limit_bytes=limit),
    )(*operands)


def read_weights(core, near, weights, keep_mask):
    half = keep_mask.shape[0] // 2
    parts = keep_mask.shape[1] // lanes
    packed = (keep_mask.shape[0] * parts, lanes)

    def kernel(
        core_ref, n_ref, g_hbm, u_hbm, d_hbm, k_hbm,
        g_ref, u_ref, d_ref, keep_ref, mask, ordered, sems,
    ):
        pairs = ((g_hbm, g_ref), (u_hbm, u_ref), (d_hbm, d_ref), (k_hbm, mask))
        moves = [pltpu.make_async_copy(*pair, sems.at[i]) for i, pair in enumerate(pairs)]
        for move in moves:
            move.start()
        moves[3].wait()
        whole = mask[...].astype(jnp.float32)
        a, b, first = whole[:half], whole[half:], core_ref[0] == 0
        for c in range(parts):
            to = slice(c * lanes, (c + 1) * lanes)
            at = 2 * half * c
            ordered[at : at + half, :] = jnp.where(first, a, b)[:, to]
            ordered[at + half : at + 2 * half, :] = jnp.where(first, b, a)[:, to]
        keep_ref[...] = ordered[...].astype(keep_ref.dtype)
        for move in moves[:3]:
            move.wait()

    space, far = (pl.BlockSpec(memory_space=m) for m in (pltpu.VMEM, pltpu.HBM))
    operands = [pltpu.with_memory_space_constraint(a, pltpu.HBM) for a in (*weights, keep_mask)]
    return pl.pallas_call(
        kernel,
        out_shape=(
            *(pltpu.VMEM(w.shape, w.dtype) for w in weights),
            pltpu.VMEM(packed, jnp.bfloat16),
        ),
        in_specs=[pl.BlockSpec(memory_space=pltpu.SMEM), space, far, far, far, far],
        out_specs=(space,) * 4,
        scratch_shapes=[
            pltpu.VMEM(keep_mask.shape, keep_mask.dtype),
            pltpu.VMEM(packed, jnp.float32),
            pltpu.SemaphoreType.DMA((4,)),
        ],
        cost_estimate=pl.CostEstimate(flops=10**9, bytes_accessed=2 << 20, transcendentals=0),
        compiler_params=pltpu.CompilerParams(vmem_limit_bytes=4 << 20),
        name="read_weights",
    )(core, near, *operands)


def collected(arrived, lost, keep):
    rows = lost.shape[0]

    def kernel(a_ref, l_ref, k_ref, sums_ref, sent_ref):
        sums = a_ref[...].astype(jnp.float32).sum(axis=0) + l_ref[...]
        sums_ref[...] = sums
        sent_ref[:rows, :] = sums.astype(sent_ref.dtype)
        sent_ref[rows:, :] = k_ref[...]

    outs = ((lost.shape, jnp.float32), ((rows + keep.shape[0], lanes), keep.dtype))
    return vmem_call(kernel, (arrived, lost, keep), outs, arrived.size)


def activations(side, sums, other, keep, ring, parts):
    total = sums.shape[0]
    half = other.shape[0] - total
    rows, half = total // parts // 3, half // parts

    def kernel(side_ref, s_ref, o_ref, k_ref, out_ref, factor):
        mine = k_ref[...].astype(jnp.float32)
        far = o_ref[total:, :].astype(jnp.float32)
        first = side_ref[0] == 0
        near, away = jnp.where(first, mine, far), jnp.where(first, far, mine)
        for c in range(parts):
            factor[:half, :] = near[half * c : half * (c + 1)]
            factor[half:, :] = away[half * c : half * (c + 1)]
            starts = [(3 * c + m) * rows for m in range(3)]
            cuts = [slice(at, at + rows) for at in starts]
            gate, up, grad = (s_ref[cut, :] + o_ref[cut, :].astype(jnp.float32) for cut in cuts)
            keep_factor = factor[...] * keep_scale
            sigmoid_gate = jax.nn.sigmoid(gate)
            silu_gate = gate * sigmoid_gate
            grad_pre = grad * keep_factor
            values = (
                silu_gate * up * keep_factor,
                grad_pre * up * sigmoid_gate * (1.0 + gate * (1.0 - sigmoid_gate)),
                grad_pre * silu_gate,
            )
            for cut, value in zip(cuts, values):
                value = value.astype(out_ref.dtype)
                for y in range(ring):
                    out_ref[y, cut, :] = value

    space, smem = (pl.BlockSpec(memory_space=m) for m in (pltpu.VMEM, pltpu.SMEM))
    operands = [pltpu.with_memory_space_constraint(a, pltpu.VMEM) for a in (sums, other, keep)]
    return pl.pallas_call(
        kernel,
        out_shape=pltpu.VMEM((ring, total, lanes), jnp.bfloat16),
        in_specs=[smem, space, space, space],
        out_specs=space,
        scratch_shapes=[pltpu.VMEM((rows, lanes), jnp.float32)],
        compiler_params=pltpu.CompilerParams(vmem_limit_bytes=4 << 20),
        name="activations",
    )(side, *operands)


def joined(ref, m, rows, parts):
    total = ref.shape[0] * rows
    cuts = [slice((3 * c + m) * rows, (3 * c + m + 1) * rows) for c in range(parts)]
    return jnp.concatenate([ref[:, cut, :].reshape(total, lanes) for cut in cuts], axis=1)


def back_products(spread, weights):
    _, _, down_weight = weights
    units, width = down_weight.shape
    parts = units // lanes
    ring, rows = spread.shape[0], spread.shape[1] // parts // 3
    total = ring * rows

    def kernel(s_ref, g_ref, u_ref, d_ref, out_ref):
        hidden, gate, up = (joined(s_ref, m, rows, parts) for m in range(3))
        out_ref[0] = dot(hidden, d_ref[...])
        out_ref[1] = dot(gate, g_ref[...], contract_last) + dot(up, u_ref[...], contract_last)

    outs = (((2, total, width), jnp.float32),)
    flops = 6 * total * width * units
    return vmem_call(kernel, (spread, *weights), outs, flops)[0]


def weight_gradients(spread, tokens, cotangent):
    total, width = tokens.shape
    ring = spread.shape[0]
    rows = total // ring
    parts = spread.shape[1] // rows // 3
    units = parts * lanes

    def kernel(s_ref, t_ref, c_ref, down_hbm, gate_hbm, up_hbm, down_ref, gate_ref, up_ref, sems):
        hidden, gate, up = (joined(s_ref, m, rows, parts) for m in range(3))
        jobs = (
            (gate_ref, gate_hbm, t_ref, gate),
            (up_ref, up_hbm, t_ref, up),
            (down_ref, down_hbm, None, None),
        )
        moves = []
        for i, (ref, hbm, x_ref, y) in enumerate(jobs):
            x, y = (hidden, c_ref[...]) if x_ref is None else (x_ref[...], y)
            ref[...] = dot(x, y, contract_first).astype(ref.dtype)
            moves.append(pltpu.make_async_copy(ref, hbm, sems.at[i]))
            moves[i].start()
        for move in moves:
            move.wait()

    kind = tokens.dtype
    outs = (((units, width), kind), ((width, units), kind), ((width, units), kind))
    scratch = [*(pltpu.VMEM(*o) for o in outs), pltpu.SemaphoreType.DMA((3,))]
    flops = 6 * total * width * units
    return vmem_call(kernel, (spread, tokens, cotangent), outs, flops, scratch, out_space=pltpu.HBM)


def own_outputs(arrived, own, width):
    def kernel(a_ref, out_ref, in_ref, flat):
        flat[...] = a_ref[...].astype(jnp.float32).sum(axis=0)
        for ref, start in ((out_ref, 0), (in_ref, flat.shape[0] // 2)):
            for c in range(width // lanes):
                piece = flat[pl.ds(start + c, own, stride=width // lanes), :]
                ref[:, c * lanes : (c + 1) * lanes] = piece.astype(ref.dtype)

    space = pl.BlockSpec(memory_space=pltpu.VMEM)
    out = jax.ShapeDtypeStruct((own, width), arrived.dtype)
    return pl.pallas_call(
        kernel,
        out_shape=(out, out),
        in_specs=[space],
        out_specs=(space, space),
        scratch_shapes=[pltpu.VMEM(arrived.shape[1:], jnp.float32)],
        compiler_params=pltpu.CompilerParams(vmem_limit_bytes=4 << 20),
        name="own_outputs",
    )(pltpu.with_memory_space_constraint(arrived, pltpu.VMEM))


def products(tokens, cotangent, weights, place, ring):
    total, units = tokens.shape[0], weights[0].shape[1]
    rows, parts = total // ring, units // lanes

    def kernel(at_ref, t_ref, c_ref, g_ref, u_ref, d_ref, out_ref, lost_ref, whole):
        own = pl.ds(pl.multiple_of(at_ref[0] * rows, rows), rows)

        def put(m, value):
            whole[...] = value
            kept = whole[own, :]
            lost = kept - kept.astype(out_ref.dtype).astype(jnp.float32)
            value = value.astype(out_ref.dtype).reshape(ring, rows, units)
            for c in range(parts):
                to = slice((3 * c + m) * rows, (3 * c + m + 1) * rows)
                out_ref[:, to, :] = value[:, :, c * lanes : (c + 1) * lanes]
                lost_ref[to, :] = lost[:, c * lanes : (c + 1) * lanes]

        put(0, dot(t_ref[...], g_ref[...]))
        put(1, dot(t_ref[...], u_ref[...]))
        put(2, dot(c_ref[...], d_ref[...], contract_last))

    space, smem = (pl.BlockSpec(memory_space=m) for m in (pltpu.VMEM, pltpu.SMEM))
    operands = (tokens, cotangent, *weights)
    operands = [pltpu.with_memory_space_constraint(a, pltpu.VMEM) for a in operands]
    return pl.pallas_call(
        kernel,
        out_shape=(
            pltpu.VMEM((ring, 3 * rows * parts, lanes), tokens.dtype),
            pltpu.VMEM((3 * rows * parts, lanes), jnp.float32),
        ),
        in_specs=[smem] + [space] * len(operands),
        out_specs=(space, space),
        scratch_shapes=[pltpu.VMEM((total, units), jnp.float32)],
        compiler_params=pltpu.CompilerParams(vmem_limit_bytes=8 << 20),
        name="products",
    )(place, *operands)


def body(tokens, gate_weight, up_weight, down_weight, keep_mask, cotangent):
    bf16 = jnp.bfloat16
    own, width = tokens.shape
    share, units = keep_mask.shape
    ring = lax.axis_size("y")
    total = share * 2 * ring
    chips = total // own // 2

    packed = jnp.concatenate([tokens, cotangent], axis=0).reshape(-1, lanes)
    half = packed.shape[0] // 2
    places = tuple(lax.axis_index(axis).reshape(1) for axis in ("core", "zh", "y"))
    packed, core, side, place = lax.optimization_barrier((packed, *places))
    near = sent_to_all(packed, plane)
    weights = (gate_weight, up_weight, down_weight)
    other = swapped(near, "core")
    *weights, keep = read_weights(core, near[0, :8], weights, keep_mask)
    both = jnp.stack([near, other], axis=1)
    all_tokens = both[:, :, :half].reshape(total, width)
    all_cot = both[:, :, half:].reshape(total, width)

    parts, lost = products(all_tokens, all_cot, weights, place, ring)
    sums, sent = collected(exchange(parts, "y"), lost, keep)
    other = swapped(sent, "zh")
    spread = exchange(activations(side, sums, other, keep, ring, units // lanes), "y")

    parts = back_products(spread, weights).reshape(2, chips, 2, -1, lanes)
    kept, given = parts[:, :, 0], parts[:, :, 1]
    other = swapped(given, "core")
    down_grad, gate_grad, up_grad = weight_gradients(spread, all_tokens, all_cot)
    parts = jnp.swapaxes((kept + other).astype(bf16), 0, 1).reshape(chips, -1, lanes)
    mixed_out, input_grad = own_outputs(exchange(parts, plane), own, width)
    return (mixed_out, input_grad, gate_grad, up_grad, down_grad)


def solution(mesh):
    fine = Mesh(mesh.devices.reshape(4, 4, 2, 8, 2), ("x", "zl", "core", "y", "zh"))
    row, col = ("x", "zl", "core"), ("y", "zh")
    by_row, by_col = P(row, col), P(col, row)

    return jax.shard_map(
        body,
        mesh=fine,
        in_specs=(by_row, by_col, by_col, by_row, by_col, by_row),
        out_specs=(by_row, by_row, by_col, by_col, by_row),
        check_vma=False,
    )
```
